256 devices in a mesh: pb: 4 (over x_hi, core), db: 64 (over x_lo, y, z).
Axes of the slice: x: 4 (x_hi: 2, x_lo: 2; x = x_hi * 2 + x_lo), y: 4, z: 8, core: 2. Of those that a mesh axis runs over, the one named last changes fastest.
Arguments:
- queries: bfloat16 [1024, 1024], P(('pb', 'db')), may hold values from -6 to 6
- residual: bfloat16 [65536, 1024], P('db'), may hold values from -3 to 3
- codes: int32 [65536, 64], P('db'), may hold values from 0 to 255
- codebook: float32 [64, 256, 16], replicated, may hold values from -6 to 6
- ranks: int32 [1024], P(('pb', 'db')), may hold values from 0 to 63
Outputs:
- hits: float32 [3, 1024], P(None, ('pb', 'db'))
- totals: float32 [3], replicated
The draws below stay inside these ranges and needn't reach their ends.
All inputs are finite; a program needn't handle non-finite values.
Results may differ from the reference program's by a relative error of at most 0.00035.
Values may be sent and summed in bfloat16 or wider, within the bound.
A program may use at most 128 MiB of HBM per device.

```python
import math
import jax
import jax.numpy as jnp
from jax import lax

SUBSPACES = 64
CENTROIDS = 256
SUBDIM = 16
D = 1024
LEVELS = 64
QUERIES = 1024
DATABASE = 65536


def draw_ranks(key, part):
    base = jax.random.randint(jax.random.fold_in(key, 7), (QUERIES,), 0, LEVELS // 4)
    rising = jnp.arange(QUERIES, dtype=jnp.int32) * (3 * LEVELS // 4) // QUERIES
    return (base + rising).astype(jnp.int32)


def place_ends(entries, own_key, low, top_value):
    index_at = [jax.random.randint(jax.random.fold_in(own_key, axis), (), 0, length) for axis, length in enumerate(entries.shape)]
    longest = entries.shape.index(max(entries.shape))
    neighbour = index_at[:longest] + [(index_at[longest] + 1) % entries.shape[longest]] + index_at[longest + 1:]
    return entries.at[tuple(index_at)].set(low).at[tuple(neighbour)].set(top_value)


def steps_of(own_key, shape, shards, low, largest):
    factor_of, own = 1.0, jax.random.fold_in(own_key, 6)
    for axis_at, shards_of in shards:
        steps = jnp.exp(jax.random.uniform(jax.random.fold_in(own, axis_at), (shards_of,), jnp.float32, low / len(shards), largest / len(shards)))
        factor_of = factor_of * jnp.repeat(steps, shape[axis_at] // shards_of).reshape([-1 if axis == axis_at else 1 for axis in range(len(shape))])
    return factor_of


def noise(key, shape, scale, reach, shards=(), kind=jnp.bfloat16):
    drawn = scale * jax.random.normal(key, shape, jnp.float32)
    if shards:
        drawn = drawn * steps_of(key, shape, shards, -0.22, 0.18)
    return jnp.clip(drawn, -reach, reach).astype(kind)


def setup_inputs(seed: int = 0) -> dict:
    seeds = jax.random.split(jax.random.key(seed), 6)
    queries = noise(seeds[0], (QUERIES, D), 1.0, 6.0, ((0, 256),))
    residual = noise(seeds[1], (DATABASE, D), 0.5, 3.0, ((0, 64),))
    codes = place_ends(jax.random.randint(seeds[2], (DATABASE, SUBSPACES), 0, CENTROIDS), jax.random.fold_in(seeds[2], 1), 0, CENTROIDS - 1).astype(jnp.int32)
    codebook = noise(seeds[3], (SUBSPACES, CENTROIDS, SUBDIM), 1.0, 6.0, (), jnp.float32)
    ranks = draw_ranks(jax.random.fold_in(seeds[5], 71), 0)
    return {"queries": queries, "residual": residual, "codes": codes, "codebook": codebook, "ranks": ranks}


def pq_lookup(queries, codebook):
    count = queries.shape[0]
    subspaces, centroids, subdim = codebook.shape
    parts = queries.astype(jnp.float32).reshape(count, subspaces, subdim)
    query_parts = jnp.sum(parts * parts, axis=-1)
    centre_norms = jnp.sum(codebook * codebook, axis=-1)
    cross = jnp.einsum("qmj,mcj->qmc", parts, codebook, precision=lax.Precision.HIGHEST)
    lookup = (query_parts[:, :, None] + centre_norms[None] - 2.0 * cross) / (subspaces * subdim)
    return lookup.astype(jnp.bfloat16)


def reference(queries, residual, codes, codebook, ranks):
    subspace_ids = jnp.arange(SUBSPACES, dtype=jnp.int32)[None, :]
    recon = codebook[subspace_ids, codes].reshape(DATABASE, D)
    vectors = (recon + residual.astype(jnp.float32)).astype(jnp.bfloat16)
    vector_norms = jnp.sum(vectors.astype(jnp.float32) ** 2, axis=1)
    bounds = 1.9 + 0.6 * ranks.astype(jnp.float32) / (LEVELS - 1)
    query_size = math.gcd(QUERIES, 128)
    base_size = math.gcd(DATABASE, 1024)
    vector_blocks = vectors.reshape(DATABASE // base_size, base_size, D)
    norm_blocks = vector_norms.reshape(DATABASE // base_size, base_size)
    code_blocks = codes.reshape(DATABASE // base_size, base_size, SUBSPACES)

    def one_block(item):
        query_block, bound_block = item
        lookup = pq_lookup(query_block, codebook)
        query_norms = jnp.sum(query_block.astype(jnp.float32) ** 2, axis=1)

        def absorb(carry, piece):
            vector_piece, norm_piece, code_piece = piece
            picked = lookup[:, subspace_ids, code_piece].astype(jnp.float32)
            coarse = jnp.sum(picked, axis=-1)
            cross = jnp.dot(query_block, vector_piece.T, preferred_element_type=jnp.float32)
            exact = (query_norms[:, None] + norm_piece[None, :] - 2.0 * cross) / D
            exact_hit = jax.nn.sigmoid((bound_block[:, None] - exact) / 0.02)
            coarse_hit = jax.nn.sigmoid((bound_block[:, None] - coarse) / 0.02)
            part_sums = jnp.stack([jnp.sum(exact_hit, 1), jnp.sum(coarse_hit, 1), jnp.sum(exact_hit * coarse_hit, 1)])
            return carry + part_sums, None

        start = jnp.zeros((3, query_block.shape[0]), jnp.float32)
        result, _ = lax.scan(absorb, start, (vector_blocks, norm_blocks, code_blocks))
        return result

    sums = lax.map(one_block, (queries.reshape(QUERIES // query_size, query_size, D), bounds.reshape(QUERIES // query_size, query_size)))
    hits = jnp.transpose(sums, (1, 0, 2)).reshape(3, QUERIES) / DATABASE
    totals = jnp.sum(hits, axis=1) / QUERIES
    return hits, totals
```

```python
import jax
import jax.numpy as jnp
from jax import lax
from jax.experimental import pallas as pl
from jax.experimental.pallas import tpu as pltpu
from jax.sharding import PartitionSpec as P

LEVELS = 64
SHARP = 50.0
LANES = 128
MESH = pl.DeviceIdType.MESH


def kernel_body(
    sizes,
    ranks_ref,
    queries_ref,
    residual_ref,
    codes_ref,
    codebook_ref,
    hits_ref,
    totals_ref,
    message,
    arrived,
    table,
    codes,
    residual,
    vectors,
    recon_high,
    recon_low,
    vector_bias,
    recon_bias,
    visiting,
    query_bias,
    sums,
    leaving,
    returned,
    own_sums,
    group_sums,
    local_sems,
    query_send,
    query_recv,
    hit_send,
    hit_recv,
    total_send,
    total_recv,
):
    db, pb, rows, width, database, everyone, subdim = sizes
    count = queries_ref.shape[0]
    me = lax.axis_index("db")
    my_pb = lax.axis_index("pb")

    loads = [
        pltpu.make_async_copy(codebook_ref, table, local_sems.at[0]),
        pltpu.make_async_copy(codes_ref, codes, local_sems.at[1]),
        pltpu.make_async_copy(residual_ref, residual, local_sems.at[2]),
    ]
    for load in loads:
        load.start()

    barrier = pltpu.get_barrier_semaphore()

    def greet(step, _):
        peer = lax.rem(me + step, db)
        pl.semaphore_signal(barrier, inc=1, device_id={"db": peer}, device_id_type=MESH)
        return 0

    lax.fori_loop(1, db, greet, 0)
    for step in range(1, pb):
        peer = lax.rem(my_pb + step, pb)
        pl.semaphore_signal(barrier, inc=1, device_id={"pb": peer}, device_id_type=MESH)

    message[:, :width] = queries_ref[...]
    row_ids = lax.broadcasted_iota(jnp.int32, (count, LANES), 0)
    rank_block = jnp.zeros((count, LANES), jnp.float32)
    for row in range(count):
        rank_block = jnp.where(row_ids == row, ranks_ref[row].astype(jnp.float32), rank_block)
    message[:, width:] = rank_block.astype(jnp.bfloat16)
    arrived[0] = message[...]

    pl.semaphore_wait(barrier, db - 1 + pb - 1)

    def send_queries(step, _):
        peer = lax.rem(me + step, db)
        pltpu.make_async_remote_copy(
            src_ref=message,
            dst_ref=arrived.at[step],
            send_sem=query_send,
            recv_sem=query_recv,
            device_id={"db": peer},
            device_id_type=MESH,
        ).start()
        return 0

    lax.fori_loop(1, db, send_queries, 0)

    for load in loads:
        load.wait()

    group = LANES // subdim

    def prepare(index, _):
        at, part = index // (width // LANES), lax.rem(index, width // LANES)
        n_at = pl.multiple_of(at * LANES, LANES)
        d_at = pl.multiple_of(part * LANES, LANES)
        extra = residual[pl.ds(n_at, LANES), pl.ds(d_at, LANES)].astype(jnp.float32).T
        chosen = codes[pl.ds(pl.multiple_of(part * group, group), group), pl.ds(n_at, LANES)]
        vector_norm = jnp.zeros((8, LANES), jnp.float32)
        recon_norm = jnp.zeros((8, LANES), jnp.float32)
        for inner in range(group):
            pick = jnp.broadcast_to(chosen[inner : inner + 1, :], (subdim, LANES))
            low_pick = pick & (LANES - 1)
            entries = table[part * group + inner]
            below = jnp.take_along_axis(
                entries[:, :LANES], low_pick, axis=1, mode="promise_in_bounds"
            )
            above = jnp.take_along_axis(
                entries[:, LANES:], low_pick, axis=1, mode="promise_in_bounds"
            )
            recon = jnp.where(pick >= LANES, above, below)
            vector = (recon + extra[inner * subdim : (inner + 1) * subdim, :]).astype(jnp.bfloat16)
            high = recon.astype(jnp.bfloat16)
            low = (recon - high.astype(jnp.float32)).astype(jnp.bfloat16)
            here = pl.ds(pl.multiple_of(d_at + inner * subdim, subdim), subdim)
            vectors[here, pl.ds(n_at, LANES)] = vector
            recon_high[here, pl.ds(n_at, LANES)] = high
            recon_low[here, pl.ds(n_at, LANES)] = low
            wide = vector.astype(jnp.float32)
            squares = wide * wide
            vector_norm += squares[:8] + squares[8:]
            squares = recon * recon
            recon_norm += squares[:8] + squares[8:]

        @pl.when(part == 0)
        def _():
            vector_bias[:, pl.ds(n_at, LANES)] = jnp.zeros((8, LANES), jnp.float32)
            recon_bias[:, pl.ds(n_at, LANES)] = jnp.zeros((8, LANES), jnp.float32)

        vector_bias[:, pl.ds(n_at, LANES)] += vector_norm
        recon_bias[:, pl.ds(n_at, LANES)] += recon_norm
        return 0

    lax.fori_loop(0, (rows // LANES) * (width // LANES), prepare, 0)

    scale = SHARP / 2
    vector_row = jnp.sum(vector_bias[...], axis=0, keepdims=True) * (-scale / width)
    recon_row = jnp.sum(recon_bias[...], axis=0, keepdims=True) * (-scale / width)
    vector_bias[...] = jnp.broadcast_to(vector_row, vector_bias.shape)
    recon_bias[...] = jnp.broadcast_to(recon_row, recon_bias.shape)

    incoming = arrived.at[pl.ds(1, db - 1)]
    pltpu.make_async_copy(incoming, incoming, query_recv).wait()

    stack = 16 // count

    def unpack(index, _):
        blocks = [arrived[index * stack + i].astype(jnp.float32) for i in range(stack)]
        block = jnp.concatenate(blocks, axis=0)
        here = pl.ds(pl.multiple_of(index * 16, 16), 16)
        own = block[:, :width]
        visiting[here, :] = own.astype(jnp.bfloat16)
        norm = jnp.sum(own * own, axis=1, keepdims=True)
        bound = 1.9 + 0.6 * block[:, width:] / (LEVELS - 1)
        query_bias[here, :] = scale * bound - (scale / width) * norm
        return 0

    lax.fori_loop(0, db // stack, unpack, 0)

    total = db * count
    sums[...] = jnp.zeros_like(sums)
    tile = 256

    def absorb(index, _):
        n_at = pl.ds(pl.multiple_of(index * tile, tile), tile)
        mine = visiting[...]
        cross = jnp.dot(mine, vectors[:, n_at], preferred_element_type=jnp.float32)
        coarse_cross = jnp.dot(mine, recon_high[:, n_at], preferred_element_type=jnp.float32)
        coarse_cross += jnp.dot(mine, recon_low[:, n_at], preferred_element_type=jnp.float32)
        bias = query_bias[...]
        for half in range(tile // LANES):
            lanes = slice(half * LANES, (half + 1) * LANES)
            row_at = pl.ds(pl.multiple_of(index * tile + half * LANES, LANES), LANES)
            exact = bias + vector_bias[0:1, row_at] + cross[:, lanes] * (2 * scale / width)
            coarse = bias + recon_bias[0:1, row_at] + coarse_cross[:, lanes] * (2 * scale / width)
            exact_hit = 0.5 * jnp.tanh(exact) + 0.5
            coarse_hit = 0.5 * jnp.tanh(coarse) + 0.5
            sums[0] += exact_hit
            sums[1] += coarse_hit
            sums[2] += exact_hit * coarse_hit
        return 0

    lax.fori_loop(0, rows // tile, absorb, 0)

    lane = lax.broadcasted_iota(jnp.int32, (total, LANES), 1)
    place = lax.rem(lax.broadcasted_iota(jnp.int32, (total, LANES), 0), count)
    spread = jnp.zeros((total, LANES), jnp.float32)
    for kind in range(3):
        column = jnp.sum(sums[kind], axis=1, keepdims=True)
        spread = jnp.where(lane == count * kind + place, column, spread)
        spread = jnp.where(lane == 3 * count + kind, column, spread)
    folder = (
        lax.broadcasted_iota(jnp.int32, (db, total), 1) // count
        == lax.broadcasted_iota(jnp.int32, (db, total), 0)
    ).astype(jnp.float32)
    folded = jnp.dot(
        folder, spread, preferred_element_type=jnp.float32, precision=lax.Precision.HIGHEST
    )
    overall = jnp.sum(spread, axis=0, keepdims=True)
    short_lane = lax.broadcasted_iota(jnp.int32, (db, LANES), 1)
    folded = jnp.where(short_lane < 3 * count, folded, overall)
    leaving[...] = folded.reshape(db, 1, LANES)
    returned[0] = folded[0:1, :]

    def send_hits(step, _):
        peer = lax.rem(me + db - step, db)
        pltpu.make_async_remote_copy(
            src_ref=leaving.at[step],
            dst_ref=returned.at[step],
            send_sem=hit_send,
            recv_sem=hit_recv,
            device_id={"db": peer},
            device_id_type=MESH,
        ).start()
        return 0

    lax.fori_loop(1, db, send_hits, 0)
    landing = returned.at[pl.ds(1, db - 1)]
    pltpu.make_async_copy(landing, landing, hit_recv).wait()
    mine = jnp.sum(returned[...], axis=0)
    own_sums[...] = mine
    for step in range(1, pb):
        pltpu.make_async_remote_copy(
            src_ref=own_sums,
            dst_ref=group_sums.at[step - 1],
            send_sem=total_send,
            recv_sem=total_recv,
            device_id={"pb": lax.rem(my_pb + step, pb)},
            device_id_type=MESH,
        ).start()
    for kind in range(3):
        hits_ref[kind : kind + 1, :] = mine[:, kind * count : (kind + 1) * count] * (1.0 / database)
    pltpu.make_async_copy(group_sums, group_sums, total_recv).wait()
    all_sums = mine + jnp.sum(group_sums[...], axis=0)
    totals_ref[...] = all_sums[:, 3 * count : 3 * count + 3] * (1.0 / (database * everyone))

    pltpu.make_async_copy(incoming, incoming, query_send).wait()
    pltpu.make_async_copy(landing, landing, hit_send).wait()
    pltpu.make_async_copy(group_sums, group_sums, total_send).wait()


def solution(mesh):
    db, pb = mesh.shape["db"], mesh.shape["pb"]

    def per_device(queries, residual, codes, codebook, ranks):
        count, width = queries.shape
        rows = residual.shape[0]
        subspaces, centroids, subdim = codebook.shape
        sizes = (db, pb, rows, width, rows * db, count * pb * db, subdim)
        total = db * count
        in_vmem = pl.BlockSpec(memory_space=pltpu.VMEM)
        anywhere = pl.BlockSpec(memory_space=pl.ANY)
        dma = pltpu.SemaphoreType.DMA
        hits, totals = pl.pallas_call(
            lambda *refs: kernel_body(sizes, *refs),
            out_shape=(
                jax.ShapeDtypeStruct((3, count), jnp.float32),
                jax.ShapeDtypeStruct((1, 3), jnp.float32),
            ),
            in_specs=[
                pl.BlockSpec(memory_space=pltpu.SMEM),
                in_vmem,
                anywhere,
                anywhere,
                anywhere,
            ],
            out_specs=(in_vmem, in_vmem),
            scratch_shapes=[
                pltpu.VMEM((count, width + LANES), jnp.bfloat16),
                pltpu.VMEM((db, count, width + LANES), jnp.bfloat16),
                pltpu.VMEM((subspaces, subdim, centroids), jnp.float32),
                pltpu.VMEM((subspaces, rows), jnp.int32),
                pltpu.VMEM((rows, width), jnp.bfloat16),
                pltpu.VMEM((width, rows), jnp.bfloat16),
                pltpu.VMEM((width, rows), jnp.bfloat16),
                pltpu.VMEM((width, rows), jnp.bfloat16),
                pltpu.VMEM((8, rows), jnp.float32),
                pltpu.VMEM((8, rows), jnp.float32),
                pltpu.VMEM((total, width), jnp.bfloat16),
                pltpu.VMEM((total, LANES), jnp.float32),
                pltpu.VMEM((3, total, LANES), jnp.float32),
                pltpu.VMEM((db, 1, LANES), jnp.float32),
                pltpu.VMEM((db, 1, LANES), jnp.float32),
                pltpu.VMEM((1, LANES), jnp.float32),
                pltpu.VMEM((pb - 1, 1, LANES), jnp.float32),
                dma((3,)),
                dma,
                dma,
                dma,
                dma,
                dma,
                dma,
            ],
            compiler_params=pltpu.CompilerParams(
                collective_id=0, has_side_effects=True, vmem_limit_bytes=60 * 1024 * 1024
            ),
            name="recall",
        )(ranks, queries, residual, codes.T, jnp.transpose(codebook, (0, 2, 1)))
        return hits, totals.reshape(3)

    return jax.shard_map(
        per_device,
        mesh=mesh,
        in_specs=(P(("pb", "db"), None), P("db", None), P("db", None), P(), P(("pb", "db"))),
        out_specs=(P(None, ("pb", "db")), P()),
        check_vma=False,
    )
```

```python
import jax
import jax.numpy as jnp
from jax import lax
from jax.experimental import pallas as pl
from jax.experimental.pallas import tpu as pltpu
from jax.sharding import PartitionSpec as P

LEVELS = 64
SHARP = 50.0
LANES = 128
MESH = pl.DeviceIdType.MESH
NX, NY, NZ = 2, 4, 8


def distance(dx, dy, dz):
    return dx + min(dy, NY - dy) + min(dz, NZ - dz)


OFFSETS = sorted(
    ((dx, dy, dz) for dx in range(NX) for dy in range(NY) for dz in range(NZ) if dx + dy + dz),
    key=lambda offset: -distance(*offset),
)
FIRST = sorted(
    ((dx, dz) for dx in range(NX) for dz in range(NZ) if dx + dz),
    key=lambda offset: distance(offset[0], 0, offset[1]),
)
PLAN = ((16, FIRST[:4]), (24, FIRST[4:8]), (32, FIRST[8:12]), (40, FIRST[12:]), (64, ()))


def kernel_body(
    sizes,
    ranks_ref,
    queries_ref,
    residual_ref,
    codes_ref,
    codebook_ref,
    result_ref,
    own_queries,
    message,
    arrived,
    table,
    codes,
    residual,
    vectors,
    recon_high,
    recon_low,
    vector_bias,
    recon_bias,
    visiting,
    query_bias,
    sums,
    leaving,
    returned,
    own_sums,
    group_sums,
    local_sems,
    query_send,
    near_recv,
    far_recv,
    hit_send,
    hit_recv,
    total_send,
    total_recv,
):
    db, pb, rows, width, database, everyone, subdim = sizes
    count = queries_ref.shape[0]
    me = lax.axis_index("db")
    my_pb = lax.axis_index("pb")

    loads = [
        pltpu.make_async_copy(queries_ref, own_queries, local_sems.at[3]),
        pltpu.make_async_copy(codebook_ref, table, local_sems.at[0]),
        pltpu.make_async_copy(codes_ref, codes, local_sems.at[1]),
        pltpu.make_async_copy(residual_ref, residual, local_sems.at[2]),
    ]
    for load in loads:
        load.start()

    my_x, my_y, my_z = lax.div(me, NY * NZ), lax.rem(lax.div(me, NZ), NY), lax.rem(me, NZ)

    def ahead(dx, dy, dz):
        x, y, z = lax.rem(my_x + dx, NX), lax.rem(my_y + dy, NY), lax.rem(my_z + dz, NZ)
        return {"db": (x * NY + y) * NZ + z}

    def behind(dx, dy, dz):
        return ahead(NX - dx, NY - dy, NZ - dz)

    barrier = pltpu.get_barrier_semaphore()
    for dx, dy, dz in OFFSETS:
        pl.semaphore_signal(barrier, inc=1, device_id=ahead(dx, dy, dz), device_id_type=MESH)
    for step in range(1, pb):
        peer = lax.rem(my_pb + step, pb)
        pl.semaphore_signal(barrier, inc=1, device_id={"pb": peer}, device_id_type=MESH)

    row_ids = lax.broadcasted_iota(jnp.int32, (count, LANES), 0)
    rank_block = jnp.zeros((count, LANES), jnp.float32)
    for row in range(count):
        rank_block = jnp.where(row_ids == row, ranks_ref[row].astype(jnp.float32), rank_block)
    message[:, width:] = rank_block.astype(jnp.bfloat16)
    loads[0].wait()
    message[:, :width] = own_queries[...]
    arrived[0] = message[...]
    vector_bias[...] = jnp.zeros_like(vector_bias)
    recon_bias[...] = jnp.zeros_like(recon_bias)

    with jax.named_scope("wait_barrier"):
        pl.semaphore_wait(barrier, db - 1 + pb - 1)

    def forward(source, slot):
        for dy in (2, 1, 3):
            pltpu.make_async_remote_copy(
                src_ref=source,
                dst_ref=arrived.at[dy * NX * NZ + slot],
                send_sem=query_send,
                recv_sem=far_recv,
                device_id=ahead(0, dy, 0),
                device_id_type=MESH,
            ).start()

    for dx, dz in FIRST:
        slot = dx * NZ + dz
        pltpu.make_async_remote_copy(
            src_ref=message,
            dst_ref=arrived.at[slot],
            send_sem=query_send,
            recv_sem=near_recv.at[slot],
            device_id=ahead(dx, 0, dz),
            device_id_type=MESH,
        ).start()
    forward(message, 0)

    group = LANES // subdim
    parts = width // LANES

    def prepare(index, _):
        at, part = lax.div(index, parts), lax.rem(index, parts)
        n_at = pl.multiple_of(at * LANES, LANES)
        d_at = pl.multiple_of(part * LANES, LANES)
        extra = residual[pl.ds(n_at, LANES), pl.ds(d_at, LANES)].T
        chosen = codes[pl.ds(pl.multiple_of(part * group, group), group), pl.ds(n_at, LANES)]
        vector_norm = jnp.zeros((8, LANES), jnp.float32)
        recon_norm = jnp.zeros((8, LANES), jnp.float32)
        for inner in range(group):
            pick = jnp.broadcast_to(chosen[inner : inner + 1, :], (subdim, LANES))
            low_pick = pick & (LANES - 1)
            entries = table[part * group + inner]
            below = jnp.take_along_axis(
                entries[:, :LANES], low_pick, axis=1, mode="promise_in_bounds"
            )
            above = jnp.take_along_axis(
                entries[:, LANES:], low_pick, axis=1, mode="promise_in_bounds"
            )
            recon = jnp.where(pick >= LANES, above, below)
            addend = extra[inner * subdim : (inner + 1) * subdim, :].astype(jnp.float32)
            vector = (recon + addend).astype(jnp.bfloat16)
            high = recon.astype(jnp.bfloat16)
            low = (recon - high.astype(jnp.float32)).astype(jnp.bfloat16)
            here = pl.ds(pl.multiple_of(d_at + inner * subdim, subdim), subdim)
            vectors[here, pl.ds(n_at, LANES)] = vector
            recon_high[here, pl.ds(n_at, LANES)] = high
            recon_low[here, pl.ds(n_at, LANES)] = low
            wide = vector.astype(jnp.float32)
            squares = wide * wide
            vector_norm += squares[:8] + squares[8:]
            squares = recon * recon
            recon_norm += squares[:8] + squares[8:]
        vector_bias[:, pl.ds(n_at, LANES)] += vector_norm
        recon_bias[:, pl.ds(n_at, LANES)] += recon_norm
        return 0

    for load in loads[1:]:
        load.wait()

    done = 0
    for upto, relays in PLAN:
        if upto > done:
            with jax.named_scope("prepare"):
                lax.fori_loop(done, upto, prepare, 0, unroll=2)
            done = upto
        with jax.named_scope("relay"):
            for dx, dz in relays:
                slot = dx * NZ + dz
                block = arrived.at[slot]
                pltpu.make_async_copy(block, block, near_recv.at[slot]).wait()
                forward(block, slot)

    scale = SHARP / 2
    vector_row = jnp.sum(vector_bias[...], axis=0, keepdims=True) * (-scale / width)
    recon_row = jnp.sum(recon_bias[...], axis=0, keepdims=True) * (-scale / width)
    vector_bias[...] = jnp.broadcast_to(vector_row, vector_bias.shape)
    recon_bias[...] = jnp.broadcast_to(recon_row, recon_bias.shape)

    incoming = arrived.at[pl.ds(NX * NZ, db - NX * NZ)]
    with jax.named_scope("wait_queries"):
        pltpu.make_async_copy(incoming, incoming, far_recv).wait()

    stack = 16 // count
    with jax.named_scope("unpack"):
        for index in range(db // stack):
            blocks = [arrived[index * stack + i].astype(jnp.float32) for i in range(stack)]
            block = jnp.concatenate(blocks, axis=0)
            here = slice(index * 16, index * 16 + 16)
            own = block[:, :width]
            visiting[here, :] = own.astype(jnp.bfloat16)
            squares = own * own
            folded = squares[:, :LANES]
            for at in range(LANES, width, LANES):
                folded += squares[:, at : at + LANES]
            norm = jnp.sum(folded, axis=1, keepdims=True)
            bound = 1.9 + 0.6 * block[:, width:] / (LEVELS - 1)
            query_bias[here, :] = scale * bound - (scale / width) * norm

    total = db * count
    sums[...] = jnp.zeros_like(sums)
    tile = 256

    def absorb(index, _):
        n_at = pl.ds(pl.multiple_of(index * tile, tile), tile)
        mine = visiting[...]
        cross = jnp.dot(mine, vectors[:, n_at], preferred_element_type=jnp.float32)
        coarse_cross = jnp.dot(mine, recon_high[:, n_at], preferred_element_type=jnp.float32)
        coarse_cross += jnp.dot(mine, recon_low[:, n_at], preferred_element_type=jnp.float32)
        bias = query_bias[...]
        for half in range(tile // LANES):
            lanes = slice(half * LANES, (half + 1) * LANES)
            row_at = pl.ds(pl.multiple_of(index * tile + half * LANES, LANES), LANES)
            exact = bias + vector_bias[0:1, row_at] + cross[:, lanes] * (2 * scale / width)
            coarse = bias + recon_bias[0:1, row_at] + coarse_cross[:, lanes] * (2 * scale / width)
            exact_hit = 0.5 * jnp.tanh(exact) + 0.5
            coarse_hit = 0.5 * jnp.tanh(coarse) + 0.5
            sums[0] += exact_hit
            sums[1] += coarse_hit
            sums[2] += exact_hit * coarse_hit
        return 0

    with jax.named_scope("absorb"):
        lax.fori_loop(0, rows // tile, absorb, 0)

    lane = lax.broadcasted_iota(jnp.int32, (total, LANES), 1)
    place = lax.rem(lax.broadcasted_iota(jnp.int32, (total, LANES), 0), count)
    spread = jnp.zeros((total, LANES), jnp.float32)
    for kind in range(3):
        column = jnp.sum(sums[kind], axis=1, keepdims=True)
        spread = jnp.where(lane == count * kind + place, column, spread)
        spread = jnp.where(lane == 3 * count + kind, column, spread)
    folder = (
        lax.broadcasted_iota(jnp.int32, (db, total), 1) // count
        == lax.broadcasted_iota(jnp.int32, (db, total), 0)
    ).astype(jnp.float32)
    folded = jnp.dot(
        folder, spread, preferred_element_type=jnp.float32, precision=lax.Precision.HIGHEST
    )
    overall = jnp.sum(spread, axis=0, keepdims=True)
    short_lane = lax.broadcasted_iota(jnp.int32, (db, LANES), 1)
    folded = jnp.where(short_lane < 3 * count, folded, overall)
    leaving[...] = folded.reshape(db, 1, LANES)
    returned[0] = folded[0:1, :]

    for dx, dy, dz in OFFSETS:
        slot = (dy * NX + dx) * NZ + dz
        pltpu.make_async_remote_copy(
            src_ref=leaving.at[slot],
            dst_ref=returned.at[slot],
            send_sem=hit_send,
            recv_sem=hit_recv,
            device_id=behind(dx, dy, dz),
            device_id_type=MESH,
        ).start()
    landing = returned.at[pl.ds(1, db - 1)]
    with jax.named_scope("wait_hits"):
        pltpu.make_async_copy(landing, landing, hit_recv).wait()
    mine = jnp.sum(returned[...], axis=0)
    own_sums[...] = mine
    for step in range(1, pb):
        pltpu.make_async_remote_copy(
            src_ref=own_sums,
            dst_ref=group_sums.at[step - 1],
            send_sem=total_send,
            recv_sem=total_recv,
            device_id={"pb": lax.rem(my_pb + step, pb)},
            device_id_type=MESH,
        ).start()
    with jax.named_scope("wait_totals"):
        pltpu.make_async_copy(group_sums, group_sums, total_recv).wait()
    all_sums = mine + jnp.sum(group_sums[...], axis=0)
    result_ref[0:1, :] = mine * (1.0 / database)
    result_ref[1:2, :] = all_sums * (1.0 / (database * everyone))

    sent = arrived.at[pl.ds(1, db - 1)]
    pltpu.make_async_copy(sent, sent, query_send).wait()
    pltpu.make_async_copy(landing, landing, hit_send).wait()
    pltpu.make_async_copy(group_sums, group_sums, total_send).wait()


def place_outputs(result_ref, hits_ref, totals_ref):
    count = hits_ref.shape[1]
    for kind in range(3):
        hits_ref[kind : kind + 1, :] = result_ref[0:1, kind * count : (kind + 1) * count]
    totals_ref[...] = result_ref[1:2, 3 * count : 3 * count + 3]


def solution(mesh):
    db, pb = mesh.shape["db"], mesh.shape["pb"]

    def per_device(queries, residual, codes, codebook, ranks):
        count, width = queries.shape
        rows = residual.shape[0]
        subspaces, centroids, subdim = codebook.shape
        sizes = (db, pb, rows, width, rows * db, count * pb * db, subdim)
        total = db * count
        in_vmem = pl.BlockSpec(memory_space=pltpu.VMEM)
        anywhere = pl.BlockSpec(memory_space=pl.ANY)
        dma = pltpu.SemaphoreType.DMA
        result = pl.pallas_call(
            lambda *refs: kernel_body(sizes, *refs),
            out_shape=jax.ShapeDtypeStruct((8, LANES), jnp.float32),
            in_specs=[pl.BlockSpec(memory_space=pltpu.SMEM)] + [anywhere] * 4,
            out_specs=in_vmem,
            scratch_shapes=[
                pltpu.VMEM((count, width), jnp.bfloat16),
                pltpu.VMEM((count, width + LANES), jnp.bfloat16),
                pltpu.VMEM((db, count, width + LANES), jnp.bfloat16),
                pltpu.VMEM((subspaces, subdim, centroids), jnp.float32),
                pltpu.VMEM((subspaces, rows), jnp.int32),
                pltpu.VMEM((rows, width), jnp.bfloat16),
                pltpu.VMEM((width, rows), jnp.bfloat16),
                pltpu.VMEM((width, rows), jnp.bfloat16),
                pltpu.VMEM((width, rows), jnp.bfloat16),
                pltpu.VMEM((8, rows), jnp.float32),
                pltpu.VMEM((8, rows), jnp.float32),
                pltpu.VMEM((total, width), jnp.bfloat16),
                pltpu.VMEM((total, LANES), jnp.float32),
                pltpu.VMEM((3, total, LANES), jnp.float32),
                pltpu.VMEM((db, 1, LANES), jnp.float32),
                pltpu.VMEM((db, 1, LANES), jnp.float32),
                pltpu.VMEM((1, LANES), jnp.float32),
                pltpu.VMEM((pb - 1, 1, LANES), jnp.float32),
                dma((4,)),
                dma,
                dma((NX * NZ,)),
                dma,
                dma,
                dma,
                dma,
                dma,
            ],
            compiler_params=pltpu.CompilerParams(
                collective_id=0, has_side_effects=True, vmem_limit_bytes=60 * 1024 * 1024
            ),
            name="recall",
        )(ranks, queries, residual, codes.T, jnp.transpose(codebook, (0, 2, 1)))
        hits, totals = pl.pallas_call(
            place_outputs,
            out_shape=(
                jax.ShapeDtypeStruct((3, count), jnp.float32),
                jax.ShapeDtypeStruct((1, 3), jnp.float32),
            ),
            name="place",
        )(result)
        return hits, totals.reshape(3)

    return jax.shard_map(
        per_device,
        mesh=mesh,
        in_specs=(P(("pb", "db"), None), P("db", None), P("db", None), P(), P(("pb", "db"))),
        out_specs=(P(None, ("pb", "db")), P()),
        check_vma=False,
    )
```

```python
import jax
import jax.numpy as jnp
from jax import lax
from jax.experimental import pallas as pl
from jax.experimental.pallas import tpu as pltpu
from jax.sharding import PartitionSpec as P

LEVELS = 64
SCALE = 25.0
LANES = 128
MESH = pl.DeviceIdType.MESH
NX, NY, NZ = 2, 4, 8
PLANE = NX * NZ


def ring(step, length):
    return min(step, length - step)


def near_first(steps):
    return sorted(steps, key=lambda step: ring(step[0], NX) + ring(step[1], NZ))


FIRST = near_first([(dx, dz) for dx in range(NX) for dz in range(NZ) if dx + dz])
ACROSS = sorted(
    ((dy, dz) for dy in range(NY) for dz in range(NZ) if dy + dz),
    key=lambda step: -ring(step[0], NY) - ring(step[1], NZ),
)
PLAN = ((16, FIRST[:4]), (24, FIRST[4:8]), (32, FIRST[8:12]), (40, FIRST[12:]), (64, ()))


def start_copy(source, target, send_sem, recv_sem, device):
    pltpu.make_async_remote_copy(
        src_ref=source,
        dst_ref=target,
        send_sem=send_sem,
        recv_sem=recv_sem,
        device_id=device,
        device_id_type=MESH,
    ).start()


def wait_bytes(block, sem):
    pltpu.make_async_copy(block, block, sem).wait()


def kernel_body(
    sizes,
    ranks_ref,
    queries_ref,
    residual_ref,
    codes_ref,
    codebook_ref,
    result_ref,
    own_ranks,
    own_queries,
    message,
    arrived,
    table,
    codes,
    residual,
    vectors,
    recons,
    vector_bias,
    recon_bias,
    visiting,
    query_bias,
    sums,
    leaving,
    returned,
    own_sums,
    side_sums,
    local_sems,
    query_send,
    near_recv,
    far_recv,
    hit_send,
    hit_recv,
    side_send,
    side_recv,
):
    db, pb, rows, width, database, everyone, subdim = sizes
    count = own_queries.shape[0]
    me = lax.axis_index("db")
    my_pb = lax.axis_index("pb")

    loads = [
        pltpu.make_async_copy(ranks_ref, own_ranks, local_sems.at[4]),
        pltpu.make_async_copy(queries_ref, own_queries, local_sems.at[3]),
        pltpu.make_async_copy(codebook_ref, table, local_sems.at[0]),
        pltpu.make_async_copy(codes_ref, codes, local_sems.at[1]),
        pltpu.make_async_copy(residual_ref, residual, local_sems.at[2]),
    ]
    for load in loads:
        load.start()

    my_x, my_y, my_z = lax.div(me, NY * NZ), lax.rem(lax.div(me, NZ), NY), lax.rem(me, NZ)

    def ahead(dx, dy, dz):
        x, y, z = lax.rem(my_x + dx, NX), lax.rem(my_y + dy, NY), lax.rem(my_z + dz, NZ)
        return (x * NY + y) * NZ + z

    def beside(dp, dx):
        return {"pb": lax.rem(my_pb + dp, pb), "db": ahead(dx, 0, 0)}

    sides = [(dp, dx) for dp in range(pb) for dx in range(NX) if dp + dx]

    barrier = pltpu.get_barrier_semaphore()
    greeted = [{"db": ahead(dx, 0, dz)} for dx, dz in FIRST[::-1]]
    greeted += [{"db": ahead(0, dy, 0)} for dy in range(1, NY)]
    greeted += [beside(dp, dx) for dp, dx in sides if dp]
    for device in greeted:
        pl.semaphore_signal(barrier, inc=1, device_id=device, device_id_type=MESH)

    row_ids = lax.broadcasted_iota(jnp.int32, (count, LANES), 0)
    rank_block = jnp.zeros((count, LANES), jnp.float32)
    loads[0].wait()
    for row in range(count):
        rank_block = jnp.where(row_ids == row, own_ranks[row].astype(jnp.float32), rank_block)
    message[:, width:] = rank_block.astype(jnp.bfloat16)
    loads[1].wait()
    message[:, :width] = own_queries[...]
    arrived[0] = message[...]
    vector_bias[...] = jnp.zeros_like(vector_bias)
    recon_bias[...] = jnp.zeros_like(recon_bias)

    with jax.named_scope("wait_barrier"):
        pl.semaphore_wait(barrier, len(greeted))

    def forward(source, slot):
        for dy in (2, 1, 3):
            start_copy(
                source,
                arrived.at[dy * PLANE + slot],
                query_send,
                far_recv.at[dy],
                {"db": ahead(0, dy, 0)},
            )

    for dx, dz in FIRST:
        slot = dx * NZ + dz
        start_copy(
            message, arrived.at[slot], query_send, near_recv.at[slot], {"db": ahead(dx, 0, dz)}
        )
    forward(message, 0)

    group = LANES // subdim
    parts = width // LANES

    def prepare(index, _):
        at, part = lax.div(index, parts), lax.rem(index, parts)
        n_at = pl.multiple_of(at * LANES, LANES)
        d_at = pl.multiple_of(part * LANES, LANES)
        extra = residual[pl.ds(n_at, LANES), pl.ds(d_at, LANES)].T
        chosen = codes[pl.ds(pl.multiple_of(part * group, group), group), pl.ds(n_at, LANES)]
        vector_norm = jnp.zeros((8, LANES), jnp.float32)
        recon_norm = jnp.zeros((8, LANES), jnp.float32)
        for inner in range(group):
            pick = jnp.broadcast_to(chosen[inner : inner + 1, :], (subdim, LANES))
            low_pick = pick & (LANES - 1)
            entries = table[part * group + inner]
            below = jnp.take_along_axis(
                entries[:, :LANES], low_pick, axis=1, mode="promise_in_bounds"
            )
            above = jnp.take_along_axis(
                entries[:, LANES:], low_pick, axis=1, mode="promise_in_bounds"
            )
            recon = jnp.where(pick >= LANES, above, below)
            addend = extra[inner * subdim : (inner + 1) * subdim, :].astype(jnp.float32)
            vector = (recon + addend).astype(jnp.bfloat16)
            here = pl.ds(pl.multiple_of(d_at + inner * subdim, subdim), subdim)
            vectors[here, pl.ds(n_at, LANES)] = vector
            recons[here, pl.ds(n_at, LANES)] = recon.astype(jnp.bfloat16)
            wide = vector.astype(jnp.float32)
            squares = wide * wide
            vector_norm += squares[:8] + squares[8:]
            squares = recon * recon
            recon_norm += squares[:8] + squares[8:]
        vector_bias[:, pl.ds(n_at, LANES)] += vector_norm
        recon_bias[:, pl.ds(n_at, LANES)] += recon_norm
        return 0

    for load in loads[2:]:
        load.wait()

    done = 0
    for upto, relays in PLAN:
        if upto > done:
            with jax.named_scope("prepare"):
                lax.fori_loop(done, upto, prepare, 0, unroll=UNROLL)
            done = upto
        with jax.named_scope("relay"):
            for dx, dz in relays:
                slot = dx * NZ + dz
                block = arrived.at[slot]
                wait_bytes(block, near_recv.at[slot])
                forward(block, slot)

    vector_row = jnp.sum(vector_bias[...], axis=0, keepdims=True) * (-SCALE / width)
    recon_row = jnp.sum(recon_bias[...], axis=0, keepdims=True) * (-SCALE / width)
    vector_bias[...] = jnp.broadcast_to(vector_row, vector_bias.shape)
    recon_bias[...] = jnp.broadcast_to(recon_row, recon_bias.shape)

    stack = 16 // count
    tile = 256
    half = 2 * PLANE * count
    sums[...] = jnp.zeros_like(sums)

    def unpack(first, last):
        for index in range(first // stack, last // stack):
            blocks = [arrived[index * stack + i].astype(jnp.float32) for i in range(stack)]
            block = jnp.concatenate(blocks, axis=0)
            here = slice(index * 16, index * 16 + 16)
            own = block[:, :width]
            visiting[here, :] = own.astype(jnp.bfloat16)
            squares = own * own
            folded = squares[:, :LANES]
            for at in range(LANES, width, LANES):
                folded += squares[:, at : at + LANES]
            norm = jnp.sum(folded, axis=1, keepdims=True)
            bound = 1.9 + 0.6 * block[:, width:] / (LEVELS - 1)
            query_bias[here, :] = SCALE * bound - (SCALE / width) * norm

    def absorb(first):
        q_at = slice(first, first + half)

        def one(index, _):
            n_at = pl.ds(pl.multiple_of(index * tile, tile), tile)
            mine = visiting[q_at, :]
            cross = jnp.dot(mine, vectors[:, n_at], preferred_element_type=jnp.float32)
            coarse_cross = jnp.dot(mine, recons[:, n_at], preferred_element_type=jnp.float32)
            bias = query_bias[q_at, :]
            parts = [0.0, 0.0, 0.0]
            for at in range(0, tile, LANES):
                row_at = pl.ds(pl.multiple_of(index * tile + at, LANES), LANES)
                lanes = slice(at, at + LANES)
                exact = bias + (vector_bias[0:1, row_at] + cross[:, lanes] * (2 * SCALE / width))
                coarse = bias + (recon_bias[0:1, row_at] + coarse_cross[:, lanes] * (2 * SCALE / width))
                exact_hit = 1.0 + jnp.tanh(exact)
                coarse_hit = 1.0 + jnp.tanh(coarse)
                parts[0] += exact_hit
                parts[1] += coarse_hit
                parts[2] += exact_hit * coarse_hit
            for kind in range(3):
                sums[kind, q_at, :] += parts[kind]
            return 0

        lax.fori_loop(0, rows // tile, one, 0, unroll=ABSORB_UNROLL)

    def plane(dy):
        return arrived.at[pl.ds(dy * PLANE, PLANE)]

    with jax.named_scope("wait_queries1"):
        wait_bytes(plane(1), far_recv.at[1])
    with jax.named_scope("unpack"):
        unpack(0, 2 * PLANE)
    with jax.named_scope("absorb"):
        absorb(0)
    with jax.named_scope("wait_queries2"):
        wait_bytes(plane(3), far_recv.at[3])
        wait_bytes(plane(2), far_recv.at[2])
    with jax.named_scope("unpack"):
        unpack(2 * PLANE, db)
    with jax.named_scope("absorb"):
        absorb(half)

    total = db * count
    lane = lax.broadcasted_iota(jnp.int32, (total, LANES), 1)
    row = lax.broadcasted_iota(jnp.int32, (total, LANES), 0)
    side_x = lax.rem(lax.div(row, NZ * count), NX)
    base = 16 * side_x + lax.rem(row, count)
    spread = jnp.zeros((total, LANES), jnp.float32)
    for kind in range(3):
        weight = 0.25 if kind == 2 else 0.5
        column = jnp.sum(sums[kind], axis=1, keepdims=True) * weight
        spread = jnp.where(lane == base + count * kind, column, spread)
        spread = jnp.where(lane == 64 + kind, column, spread)
    out_row = lax.broadcasted_iota(jnp.int32, (NY * NZ, total), 0)
    from_row = lax.broadcasted_iota(jnp.int32, (NY * NZ, total), 1)
    from_slot = lax.div(from_row, count)
    from_place = lax.div(from_slot, PLANE) * NZ + lax.rem(from_slot, NZ)
    folder = (from_place == out_row).astype(jnp.float32)
    folded = jnp.dot(
        folder, spread, preferred_element_type=jnp.float32, precision=lax.Precision.HIGHEST
    )
    overall = jnp.sum(spread, axis=0, keepdims=True)
    short_lane = lax.broadcasted_iota(jnp.int32, (NY * NZ, LANES), 1)
    folded = jnp.where(short_lane < 64, folded, overall)
    leaving[...] = folded.reshape(NY * NZ, 1, LANES)
    returned[0] = folded[0:1, :]

    for dy, dz in ACROSS:
        place = dy * NZ + dz
        start_copy(
            leaving.at[place],
            returned.at[place],
            hit_send,
            hit_recv,
            {"db": ahead(0, NY - dy, NZ - dz)},
        )
    landing = returned.at[pl.ds(1, NY * NZ - 1)]
    with jax.named_scope("wait_hits"):
        wait_bytes(landing, hit_recv)
    mine = jnp.sum(returned[...], axis=0)
    own_sums[...] = mine
    for place, (dp, dx) in enumerate(sides):
        start_copy(own_sums, side_sums.at[place], side_send, side_recv, beside(dp, dx))
    with jax.named_scope("wait_totals"):
        wait_bytes(side_sums, side_recv)
    all_sums = mine + jnp.sum(side_sums[...], axis=0)
    partner = side_sums[sides.index((0, 1))]
    result_ref[0:1, :] = mine * (1.0 / database)
    result_ref[1:2, :] = partner * (1.0 / database)
    result_ref[2:3, :] = all_sums * (1.0 / (database * everyone))

    sent = arrived.at[pl.ds(1, db - 1)]
    wait_bytes(sent, query_send)
    wait_bytes(landing, hit_send)
    wait_bytes(side_sums, side_send)


UNROLL = 4
ABSORB_UNROLL = 2


def place_outputs(result_ref, hits_ref, totals_ref):
    count = hits_ref.shape[1]
    for kind in range(3):
        first = result_ref[0:1, kind * count : (kind + 1) * count]
        second = result_ref[1:2, 16 + kind * count : 16 + (kind + 1) * count]
        hits_ref[kind : kind + 1, :] = first + second
    totals_ref[...] = result_ref[2:3, 64:67]


def solution(mesh):
    db, pb = mesh.shape["db"], mesh.shape["pb"]

    def per_device(queries, residual, codes, codebook, ranks):
        count, width = queries.shape
        rows = residual.shape[0]
        subspaces, centroids, subdim = codebook.shape
        sizes = (db, pb, rows, width, rows * db, count * pb * db, subdim)
        total = db * count
        in_vmem = pl.BlockSpec(memory_space=pltpu.VMEM)
        anywhere = pl.BlockSpec(memory_space=pl.ANY)
        dma = pltpu.SemaphoreType.DMA
        result = pl.pallas_call(
            lambda *refs: kernel_body(sizes, *refs),
            out_shape=pltpu.VMEM((8, LANES), jnp.float32),
            in_specs=[anywhere] * 5,
            out_specs=in_vmem,
            scratch_shapes=[
                pltpu.SMEM((count,), jnp.int32),
                pltpu.VMEM((count, width), jnp.bfloat16),
                pltpu.VMEM((count, width + LANES), jnp.bfloat16),
                pltpu.VMEM((db, count, width + LANES), jnp.bfloat16),
                pltpu.VMEM((subspaces, subdim, centroids), jnp.float32),
                pltpu.VMEM((subspaces, rows), jnp.int32),
                pltpu.VMEM((rows, width), jnp.bfloat16),
                pltpu.VMEM((width, rows), jnp.bfloat16),
                pltpu.VMEM((width, rows), jnp.bfloat16),
                pltpu.VMEM((8, rows), jnp.float32),
                pltpu.VMEM((8, rows), jnp.float32),
                pltpu.VMEM((total, width), jnp.bfloat16),
                pltpu.VMEM((total, LANES), jnp.float32),
                pltpu.VMEM((3, total, LANES), jnp.float32),
                pltpu.VMEM((NY * NZ, 1, LANES), jnp.float32),
                pltpu.VMEM((NY * NZ, 1, LANES), jnp.float32),
                pltpu.VMEM((1, LANES), jnp.float32),
                pltpu.VMEM((pb * NX - 1, 1, LANES), jnp.float32),
                dma((5,)),
                dma,
                dma((PLANE,)),
                dma((NY,)),
                dma,
                dma,
                dma,
                dma,
            ],
            compiler_params=pltpu.CompilerParams(
                collective_id=0, has_side_effects=True, vmem_limit_bytes=60 * 1024 * 1024
            ),
            name="recall",
        )(ranks, queries, residual, codes.T, jnp.transpose(codebook, (0, 2, 1)))
        hits, totals = pl.pallas_call(
            place_outputs,
            out_shape=(
                jax.ShapeDtypeStruct((3, count), jnp.float32),
                jax.ShapeDtypeStruct((1, 3), jnp.float32),
            ),
            in_specs=[in_vmem],
            name="place",
        )(pltpu.with_memory_space_constraint(result, pltpu.VMEM))
        return hits, totals.reshape(3)

    return jax.shard_map(
        per_device,
        mesh=mesh,
        in_specs=(P(("pb", "db"), None), P("db", None), P("db", None), P(), P(("pb", "db"))),
        out_specs=(P(None, ("pb", "db")), P()),
        check_vma=False,
    )
```

```python
import jax
import jax.numpy as jnp
from jax import lax
from jax.experimental import pallas as pl
from jax.experimental.pallas import tpu as pltpu
from jax.sharding import PartitionSpec as P

LEVELS = 64
SCALE = 25.0
LANES = 128
MESH = pl.DeviceIdType.MESH
NX, NY, NZ = 2, 4, 8
PLANE = NX * NY
FIRST_COLUMNS = 768
Z_STEPS = (0, 1, 7, 2, 6, 3, 5, 4)
XY_STEPS = ((0, 0), (0, 1), (0, 3), (1, 0), (1, 1), (1, 3), (0, 2), (1, 2))


def ring(step, length):
    return min(step, length - step)


ACROSS = sorted(
    ((dy, at) for dy in range(NY) for at in range(NZ) if dy + at),
    key=lambda step: -ring(step[0], NY) - ring(Z_STEPS[step[1]], NZ),
)
PLAN = ((16, (1, 2), (1, 2, 3)), (20, (3, 4), (4, 5, 6)), (24, (5, 6), (7,)), (28, (7,), ()), (64, (), ()))


def lane_gather(rows, index):
    numbers = lax.GatherDimensionNumbers(
        offset_dims=(),
        collapsed_slice_dims=(1,),
        start_index_map=(1,),
        operand_batching_dims=(0,),
        start_indices_batching_dims=(0,),
    )
    return lax.gather(
        rows,
        index[:, :, None],
        dimension_numbers=numbers,
        slice_sizes=(1, 1),
        mode=lax.GatherScatterMode.PROMISE_IN_BOUNDS,
    )


def start_copy(source, target, send_sem, recv_sem, device):
    pltpu.make_async_remote_copy(
        src_ref=source,
        dst_ref=target,
        send_sem=send_sem,
        recv_sem=recv_sem,
        device_id=device,
        device_id_type=MESH,
    ).start()


def wait_bytes(block, sem):
    pltpu.make_async_copy(block, block, sem).wait()


def kernel_body(
    sizes,
    ranks_ref,
    queries_ref,
    residual_ref,
    codes_ref,
    codebook_ref,
    result_ref,
    own_ranks,
    own_queries,
    message,
    arrived,
    table,
    codes,
    residual,
    vectors,
    recons,
    vector_bias,
    recon_bias,
    visiting,
    query_bias,
    sums,
    lane_place,
    folder,
    leaving,
    returned,
    own_sums,
    side_sums,
    local_sems,
    query_send,
    near_first,
    near_second,
    far_first,
    far_second,
    hit_send,
    hit_recv,
    side_send,
    side_recv,
):
    db, pb, rows, width, database, everyone, subdim = sizes
    count = own_queries.shape[0]
    me = lax.axis_index("db")
    my_pb = lax.axis_index("pb")

    loads = [
        pltpu.make_async_copy(ranks_ref, own_ranks, local_sems.at[4]),
        pltpu.make_async_copy(queries_ref, own_queries, local_sems.at[3]),
        pltpu.make_async_copy(codebook_ref, table, local_sems.at[0]),
        pltpu.make_async_copy(codes_ref, codes, local_sems.at[1]),
        pltpu.make_async_copy(residual_ref, residual, local_sems.at[2]),
    ]
    for load in loads:
        load.start()

    my_x, my_y, my_z = lax.div(me, NY * NZ), lax.rem(lax.div(me, NZ), NY), lax.rem(me, NZ)

    def ahead(dx, dy, dz):
        x, y, z = lax.rem(my_x + dx, NX), lax.rem(my_y + dy, NY), lax.rem(my_z + dz, NZ)
        return (x * NY + y) * NZ + z

    def beside(dp, dx):
        return {"pb": lax.rem(my_pb + dp, pb), "db": ahead(dx, 0, 0)}

    sides = [(dp, dx) for dp in range(pb) for dx in range(NX) if dp + dx]

    barrier = pltpu.get_barrier_semaphore()
    greeted = [{"db": ahead(0, 0, dz)} for dz in Z_STEPS[:0:-1]]
    greeted += [{"db": ahead(dx, dy, 0)} for dx, dy in XY_STEPS[:0:-1]]
    greeted += [beside(dp, dx) for dp, dx in sides if dp]
    for device in greeted:
        pl.semaphore_signal(barrier, inc=1, device_id=device, device_id_type=MESH)

    row_ids = lax.broadcasted_iota(jnp.int32, (count, LANES), 0)
    rank_block = jnp.zeros((count, LANES), jnp.float32)
    loads[0].wait()
    for row in range(count):
        rank_block = jnp.where(row_ids == row, own_ranks[row].astype(jnp.float32), rank_block)
    message[:, width:] = rank_block.astype(jnp.bfloat16)
    loads[1].wait()
    message[:, :width] = own_queries[...]
    arrived[0] = message[...]
    vector_bias[...] = jnp.zeros_like(vector_bias)
    recon_bias[...] = jnp.zeros_like(recon_bias)

    with jax.named_scope("wait_barrier"):
        pl.semaphore_wait(barrier, len(greeted))

    first_part, second_part = pl.ds(0, FIRST_COLUMNS), pl.ds(FIRST_COLUMNS, width + LANES - FIRST_COLUMNS)
    half_steps = NZ // 2

    def send_xy(source, at):
        for group_at in range(PLANE - 1, 0, -1):
            dx, dy = XY_STEPS[group_at]
            start_copy(
                source,
                arrived.at[at * PLANE + group_at, :, first_part],
                query_send,
                far_first.at[at // half_steps],
                {"db": ahead(dx, dy, 0)},
            )

    def send_z(source, group_at):
        for at in range(NZ - 1, 0, -1):
            start_copy(
                source,
                arrived.at[at * PLANE + group_at, :, second_part],
                query_send,
                far_second.at[at // half_steps],
                {"db": ahead(0, 0, Z_STEPS[at])},
            )

    for at in range(1, NZ):
        start_copy(
            message.at[:, first_part],
            arrived.at[at * PLANE, :, first_part],
            query_send,
            near_first.at[at],
            {"db": ahead(0, 0, Z_STEPS[at])},
        )
    for group_at in range(1, PLANE):
        dx, dy = XY_STEPS[group_at]
        start_copy(
            message.at[:, second_part],
            arrived.at[group_at, :, second_part],
            query_send,
            near_second.at[group_at],
            {"db": ahead(dx, dy, 0)},
        )
    send_xy(message.at[:, first_part], 0)
    send_z(message.at[:, second_part], 0)

    group = LANES // subdim
    parts = width // LANES

    def prepare(index, _):
        at, part = lax.div(index, parts), lax.rem(index, parts)
        n_at = pl.multiple_of(at * LANES, LANES)
        d_at = pl.multiple_of(part * LANES, LANES)
        extra = residual[pl.ds(n_at, LANES), pl.ds(d_at, LANES)].T
        chosen = codes[pl.ds(pl.multiple_of(part * group, group), group), pl.ds(n_at, LANES)]
        vector_norm = jnp.zeros((8, LANES), jnp.float32)
        recon_norm = jnp.zeros((8, LANES), jnp.float32)
        for inner in range(group):
            pick = jnp.broadcast_to(chosen[inner : inner + 1, :], (subdim, LANES))
            low_pick = pick & (LANES - 1)
            entries = table[part * group + inner]
            below = lane_gather(entries[:, :LANES], low_pick)
            above = lane_gather(entries[:, LANES:], low_pick)
            recon = jnp.where(pick >= LANES, above, below)
            addend = extra[inner * subdim : (inner + 1) * subdim, :].astype(jnp.float32)
            vector = (recon + addend).astype(jnp.bfloat16)
            here = pl.ds(pl.multiple_of(d_at + inner * subdim, subdim), subdim)
            vectors[here, pl.ds(n_at, LANES)] = vector
            recons[here, pl.ds(n_at, LANES)] = recon.astype(jnp.bfloat16)
            wide = vector.astype(jnp.float32)
            squares = wide * wide
            vector_norm += squares[:8] + squares[8:]
            squares = recon * recon
            recon_norm += squares[:8] + squares[8:]
        vector_bias[:, pl.ds(n_at, LANES)] += vector_norm
        recon_bias[:, pl.ds(n_at, LANES)] += recon_norm
        return 0

    for load in loads[2:]:
        load.wait()

    done = 0
    for upto, z_arrivals, xy_arrivals in PLAN:
        with jax.named_scope("prepare"):
            lax.fori_loop(done, upto, prepare, 0, unroll=UNROLL)
        done = upto
        with jax.named_scope("relay"):
            for at in z_arrivals:
                block = arrived.at[at * PLANE, :, first_part]
                wait_bytes(block, near_first.at[at])
                send_xy(block, at)
            for group_at in xy_arrivals:
                block = arrived.at[group_at, :, second_part]
                wait_bytes(block, near_second.at[group_at])
                send_z(block, group_at)

    total = db * count
    lane = lax.broadcasted_iota(jnp.int32, (total, LANES), 1)
    row = lax.broadcasted_iota(jnp.int32, (total, LANES), 0)
    row_group = lax.rem(lax.div(row, count), PLANE)
    base = lax.rem(row, count)
    for group_at, (dx, dy) in enumerate(XY_STEPS):
        if dx:
            base = jnp.where(row_group == group_at, base + 16, base)
    lane_place[...] = lane - base
    out_row = lax.broadcasted_iota(jnp.int32, (NY * NZ, total), 0)
    from_row = lax.broadcasted_iota(jnp.int32, (NY * NZ, total), 1)
    from_group = lax.rem(lax.div(from_row, count), PLANE)
    from_place = lax.div(from_row, PLANE * count)
    for group_at, (dx, dy) in enumerate(XY_STEPS):
        if dy:
            from_place = jnp.where(from_group == group_at, from_place + dy * NZ, from_place)
    folder[...] = (from_place == out_row).astype(jnp.float32).astype(jnp.bfloat16)

    vector_row = jnp.sum(vector_bias[...], axis=0, keepdims=True) * (-SCALE / width)
    recon_row = jnp.sum(recon_bias[...], axis=0, keepdims=True) * (-SCALE / width)
    vector_bias[...] = jnp.broadcast_to(vector_row, vector_bias.shape)
    recon_bias[...] = jnp.broadcast_to(recon_row, recon_bias.shape)

    stack = 16 // count
    tile = 256
    half = half_steps * PLANE * count
    sums[...] = jnp.zeros_like(sums)

    def unpack(first, last):
        for index in range(first // stack, last // stack):
            blocks = [arrived[index * stack + i].astype(jnp.float32) for i in range(stack)]
            block = jnp.concatenate(blocks, axis=0)
            here = slice(index * 16, index * 16 + 16)
            own = block[:, :width]
            visiting[here, :] = own.astype(jnp.bfloat16)
            squares = own * own
            folded = squares[:, :LANES]
            for at in range(LANES, width, LANES):
                folded += squares[:, at : at + LANES]
            norm = jnp.sum(folded, axis=1, keepdims=True)
            bound = 1.9 + 0.6 * block[:, width:] / (LEVELS - 1)
            query_bias[here, :] = SCALE * bound - (SCALE / width) * norm

    def absorb(first):
        q_at = slice(first, first + half)

        def one(index, _):
            n_at = pl.ds(pl.multiple_of(index * tile, tile), tile)
            mine = visiting[q_at, :]
            cross = jnp.dot(mine, vectors[:, n_at], preferred_element_type=jnp.float32)
            coarse_cross = jnp.dot(mine, recons[:, n_at], preferred_element_type=jnp.float32)
            bias = query_bias[q_at, :]
            parts = [0.0, 0.0, 0.0]
            for at in range(0, tile, LANES):
                row_at = pl.ds(pl.multiple_of(index * tile + at, LANES), LANES)
                lanes = slice(at, at + LANES)
                exact = bias + (vector_bias[0:1, row_at] + cross[:, lanes] * (2 * SCALE / width))
                coarse = bias + (recon_bias[0:1, row_at] + coarse_cross[:, lanes] * (2 * SCALE / width))
                exact_hit = 1.0 + jnp.tanh(exact)
                coarse_hit = 1.0 + jnp.tanh(coarse)
                parts[0] += exact_hit
                parts[1] += coarse_hit
                parts[2] += exact_hit * coarse_hit
            for kind in range(3):
                sums[kind, q_at, :] += parts[kind]
            return 0

        lax.fori_loop(0, rows // tile, one, 0, unroll=ABSORB_UNROLL)

    def wait_half(which):
        steps = half_steps - 1 + which
        first_span = pl.ds(which * half_steps * PLANE + 1, half_steps * (PLANE - 1))
        wait_bytes(arrived.at[first_span, :, first_part], far_first.at[which])
        start = half_steps if which else 1
        second_span = pl.ds(start * PLANE, steps * PLANE)
        wait_bytes(arrived.at[second_span, :, second_part], far_second.at[which])

    with jax.named_scope("wait_queries1"):
        wait_half(0)
    with jax.named_scope("unpack"):
        unpack(0, half_steps * PLANE)
    with jax.named_scope("absorb"):
        absorb(0)
    with jax.named_scope("wait_queries2"):
        wait_half(1)
    with jax.named_scope("unpack"):
        unpack(half_steps * PLANE, db)
    with jax.named_scope("absorb"):
        absorb(half)

    spread = jnp.zeros((total, LANES), jnp.float32)
    place = lane_place[...]
    overall = []
    for kind in range(3):
        weight = 0.25 if kind == 2 else 0.5
        column = jnp.sum(sums[kind], axis=1, keepdims=True) * weight
        spread = jnp.where(place == count * kind, column, spread)
        overall.append(jnp.sum(column, axis=0, keepdims=True))
    rest, folded = spread, 0.0
    for _ in range(3):
        piece = rest.astype(jnp.bfloat16)
        rest = rest - piece.astype(jnp.float32)
        folded += jnp.dot(folder[...], piece, preferred_element_type=jnp.float32)
    short_lane = lax.broadcasted_iota(jnp.int32, (NY * NZ, LANES), 1)
    for kind in range(3):
        folded = jnp.where(short_lane == 64 + kind, overall[kind], folded)
    leaving[...] = folded.reshape(NY * NZ, 1, LANES)
    returned[0] = folded[0:1, :]

    for dy, at in ACROSS:
        place = dy * NZ + at
        start_copy(
            leaving.at[place],
            returned.at[place],
            hit_send,
            hit_recv,
            {"db": ahead(0, NY - dy, NZ - Z_STEPS[at])},
        )
    landing = returned.at[pl.ds(1, NY * NZ - 1)]
    with jax.named_scope("wait_hits"):
        wait_bytes(landing, hit_recv)
    mine = jnp.sum(returned[...], axis=0)
    own_sums[...] = mine
    for place, (dp, dx) in enumerate(sides):
        start_copy(own_sums, side_sums.at[place], side_send, side_recv, beside(dp, dx))
    with jax.named_scope("wait_totals"):
        wait_bytes(side_sums, side_recv)
    all_sums = mine + jnp.sum(side_sums[...], axis=0)
    partner = side_sums[sides.index((0, 1))]
    result_ref[0:1, :] = mine * (1.0 / database)
    result_ref[1:2, :] = partner * (1.0 / database)
    result_ref[2:3, :] = all_sums * (1.0 / (database * everyone))

    sent = arrived.at[pl.ds(1, db - 1)]
    wait_bytes(sent, query_send)
    wait_bytes(landing, hit_send)
    wait_bytes(side_sums, side_send)


UNROLL = 4
ABSORB_UNROLL = 4


def place_outputs(result_ref, hits_ref, totals_ref):
    count = hits_ref.shape[1]
    for kind in range(3):
        first = result_ref[0:1, kind * count : (kind + 1) * count]
        second = result_ref[1:2, 16 + kind * count : 16 + (kind + 1) * count]
        hits_ref[kind : kind + 1, :] = first + second
    totals_ref[...] = result_ref[2:3, 64:67]


def solution(mesh):
    db, pb = mesh.shape["db"], mesh.shape["pb"]

    def per_device(queries, residual, codes, codebook, ranks):
        count, width = queries.shape
        rows = residual.shape[0]
        subspaces, centroids, subdim = codebook.shape
        sizes = (db, pb, rows, width, rows * db, count * pb * db, subdim)
        total = db * count
        in_vmem = pl.BlockSpec(memory_space=pltpu.VMEM)
        anywhere = pl.BlockSpec(memory_space=pl.ANY)
        dma = pltpu.SemaphoreType.DMA
        result = pl.pallas_call(
            lambda *refs: kernel_body(sizes, *refs),
            out_shape=pltpu.VMEM((8, LANES), jnp.float32),
            in_specs=[anywhere] * 5,
            out_specs=in_vmem,
            scratch_shapes=[
                pltpu.SMEM((count,), jnp.int32),
                pltpu.VMEM((count, width), jnp.bfloat16),
                pltpu.VMEM((count, width + LANES), jnp.bfloat16),
                pltpu.VMEM((db, count, width + LANES), jnp.bfloat16),
                pltpu.VMEM((subspaces, subdim, centroids), jnp.float32),
                pltpu.VMEM((subspaces, rows), jnp.int32),
                pltpu.VMEM((rows, width), jnp.bfloat16),
                pltpu.VMEM((width, rows), jnp.bfloat16),
                pltpu.VMEM((width, rows), jnp.bfloat16),
                pltpu.VMEM((8, rows), jnp.float32),
                pltpu.VMEM((8, rows), jnp.float32),
                pltpu.VMEM((total, width), jnp.bfloat16),
                pltpu.VMEM((total, LANES), jnp.float32),
                pltpu.VMEM((3, total, LANES), jnp.float32),
                pltpu.VMEM((total, LANES), jnp.int32),
                pltpu.VMEM((NY * NZ, total), jnp.bfloat16),
                pltpu.VMEM((NY * NZ, 1, LANES), jnp.float32),
                pltpu.VMEM((NY * NZ, 1, LANES), jnp.float32),
                pltpu.VMEM((1, LANES), jnp.float32),
                pltpu.VMEM((pb * NX - 1, 1, LANES), jnp.float32),
                dma((5,)),
                dma,
                dma((NZ,)),
                dma((PLANE,)),
                dma((2,)),
                dma((2,)),
                dma,
                dma,
                dma,
                dma,
            ],
            compiler_params=pltpu.CompilerParams(
                collective_id=0, has_side_effects=True, vmem_limit_bytes=60 * 1024 * 1024
            ),
            name="recall",
        )(ranks, queries, residual, codes.T, jnp.transpose(codebook, (0, 2, 1)))
        hits, totals = pl.pallas_call(
            place_outputs,
            out_shape=(
                jax.ShapeDtypeStruct((3, count), jnp.float32),
                jax.ShapeDtypeStruct((1, 3), jnp.float32),
            ),
            in_specs=[in_vmem],
            name="place",
        )(pltpu.with_memory_space_constraint(result, pltpu.VMEM))
        return hits, totals.reshape(3)

    return jax.shard_map(
        per_device,
        mesh=mesh,
        in_specs=(P(("pb", "db"), None), P("db", None), P("db", None), P(), P(("pb", "db"))),
        out_specs=(P(None, ("pb", "db")), P()),
        check_vma=False,
    )
```

```python
import jax
import jax.numpy as jnp
from jax import lax
from jax.experimental import pallas as pl
from jax.experimental.pallas import tpu as pltpu
from jax.sharding import PartitionSpec as P

LEVELS = 64
SCALE = 25.0
LANES = 128
MESH = pl.DeviceIdType.MESH
NX, NY, NZ = 2, 4, 8
PLANE = NX * NY
FIRST_COLUMNS = 768
Z_STEPS = (0, 1, 7, 2, 6, 3, 5, 4)
XY_STEPS = ((0, 0), (0, 1), (0, 3), (1, 0), (1, 1), (1, 3), (0, 2), (1, 2))


def ring(step, length):
    return min(step, length - step)


ACROSS = sorted(
    ((dy, at) for dy in range(NY) for at in range(NZ) if dy + at),
    key=lambda step: -ring(step[0], NY) - ring(Z_STEPS[step[1]], NZ),
)
PLAN = ((16, (1, 2), (1, 2, 3)), (20, (3, 4), (4, 5, 6)), (24, (5, 6), (7,)), (28, (7,), ()), (64, (), ()))


def lane_gather(rows, index):
    numbers = lax.GatherDimensionNumbers(
        offset_dims=(),
        collapsed_slice_dims=(1,),
        start_index_map=(1,),
        operand_batching_dims=(0,),
        start_indices_batching_dims=(0,),
    )
    return lax.gather(
        rows,
        index[:, :, None],
        dimension_numbers=numbers,
        slice_sizes=(1, 1),
        mode=lax.GatherScatterMode.PROMISE_IN_BOUNDS,
    )


def start_copy(source, target, send_sem, recv_sem, device):
    pltpu.make_async_remote_copy(
        src_ref=source,
        dst_ref=target,
        send_sem=send_sem,
        recv_sem=recv_sem,
        device_id=device,
        device_id_type=MESH,
    ).start()


def wait_bytes(block, sem):
    pltpu.make_async_copy(block, block, sem).wait()


def kernel_body(
    sizes,
    ranks_ref,
    queries_ref,
    residual_ref,
    codes_ref,
    codebook_ref,
    result_ref,
    own_ranks,
    own_queries,
    message,
    arrived,
    table,
    codes,
    residual,
    vectors,
    recons,
    vector_bias,
    recon_bias,
    visiting,
    query_bias,
    sums,
    lane_place,
    spreads,
    folder,
    leaving,
    returned,
    own_sums,
    side_sums,
    local_sems,
    query_send,
    near_first,
    near_second,
    far_first,
    far_second,
    hit_send,
    hit_recv,
    side_send,
    side_recv,
):
    db, pb, rows, width, database, everyone, subdim = sizes
    count = own_queries.shape[0]
    me = lax.axis_index("db")
    my_pb = lax.axis_index("pb")

    loads = [
        pltpu.make_async_copy(ranks_ref, own_ranks, local_sems.at[4]),
        pltpu.make_async_copy(queries_ref, own_queries, local_sems.at[3]),
        pltpu.make_async_copy(codebook_ref, table, local_sems.at[0]),
        pltpu.make_async_copy(codes_ref, codes, local_sems.at[1]),
        pltpu.make_async_copy(residual_ref, residual, local_sems.at[2]),
    ]

    my_x, my_y, my_z = lax.div(me, NY * NZ), lax.rem(lax.div(me, NZ), NY), lax.rem(me, NZ)

    def ahead(dx, dy, dz):
        x, y, z = lax.rem(my_x + dx, NX), lax.rem(my_y + dy, NY), lax.rem(my_z + dz, NZ)
        return (x * NY + y) * NZ + z

    def beside(dp, dx):
        return {"pb": lax.rem(my_pb + dp, pb), "db": ahead(dx, 0, 0)}

    sides = [(dp, dx) for dp in range(pb) for dx in range(NX) if dp + dx]

    barrier = pltpu.get_barrier_semaphore()
    greeted = [{"db": ahead(0, 0, dz)} for dz in Z_STEPS[:0:-1]]
    greeted += [{"db": ahead(dx, dy, 0)} for dx, dy in XY_STEPS[:0:-1]]
    greeted += [beside(dp, dx) for dp, dx in sides if dp]
    for device in greeted:
        pl.semaphore_signal(barrier, inc=1, device_id=device, device_id_type=MESH)
    for load in loads:
        load.start()

    row_ids = lax.broadcasted_iota(jnp.int32, (count, LANES), 0)
    rank_block = jnp.zeros((count, LANES), jnp.float32)
    loads[0].wait()
    for row in range(count):
        rank_block = jnp.where(row_ids == row, own_ranks[row].astype(jnp.float32), rank_block)
    message[:, width:] = rank_block.astype(jnp.bfloat16)
    loads[1].wait()
    message[:, :width] = own_queries[...]
    arrived[0] = message[...]
    vector_bias[...] = jnp.zeros_like(vector_bias)
    recon_bias[...] = jnp.zeros_like(recon_bias)

    with jax.named_scope("wait_barrier"):
        pl.semaphore_wait(barrier, len(greeted))

    first_part, second_part = pl.ds(0, FIRST_COLUMNS), pl.ds(FIRST_COLUMNS, width + LANES - FIRST_COLUMNS)
    half_steps = NZ // 2

    def send_xy(source, at):
        for group_at in range(PLANE - 1, 0, -1):
            dx, dy = XY_STEPS[group_at]
            start_copy(
                source,
                arrived.at[at * PLANE + group_at, :, first_part],
                query_send,
                far_first.at[at // half_steps],
                {"db": ahead(dx, dy, 0)},
            )

    def send_z(source, group_at):
        for at in range(NZ - 1, 0, -1):
            start_copy(
                source,
                arrived.at[at * PLANE + group_at, :, second_part],
                query_send,
                far_second.at[at // half_steps],
                {"db": ahead(0, 0, Z_STEPS[at])},
            )

    for at in range(1, NZ):
        start_copy(
            message.at[:, first_part],
            arrived.at[at * PLANE, :, first_part],
            query_send,
            near_first.at[at],
            {"db": ahead(0, 0, Z_STEPS[at])},
        )
    for group_at in range(1, PLANE):
        dx, dy = XY_STEPS[group_at]
        start_copy(
            message.at[:, second_part],
            arrived.at[group_at, :, second_part],
            query_send,
            near_second.at[group_at],
            {"db": ahead(dx, dy, 0)},
        )
    send_xy(message.at[:, first_part], 0)
    send_z(message.at[:, second_part], 0)

    group = LANES // subdim
    parts = width // LANES

    def prepare(index, _):
        at, part = lax.div(index, parts), lax.rem(index, parts)
        n_at = pl.multiple_of(at * LANES, LANES)
        d_at = pl.multiple_of(part * LANES, LANES)
        extra = residual[pl.ds(n_at, LANES), pl.ds(d_at, LANES)].T
        chosen = codes[pl.ds(pl.multiple_of(part * group, group), group), pl.ds(n_at, LANES)]
        vector_norm = jnp.zeros((8, LANES), jnp.float32)
        recon_norm = jnp.zeros((8, LANES), jnp.float32)
        for inner in range(group):
            pick = jnp.broadcast_to(chosen[inner : inner + 1, :], (subdim, LANES))
            low_pick = pick & (LANES - 1)
            entries = table[part * group + inner]
            below = lane_gather(entries[:, :LANES], low_pick)
            above = lane_gather(entries[:, LANES:], low_pick)
            recon = jnp.where(pick >= LANES, above, below)
            addend = extra[inner * subdim : (inner + 1) * subdim, :].astype(jnp.float32)
            vector = (recon + addend).astype(jnp.bfloat16)
            here = pl.ds(pl.multiple_of(d_at + inner * subdim, subdim), subdim)
            vectors[here, pl.ds(n_at, LANES)] = vector
            recons[here, pl.ds(n_at, LANES)] = recon.astype(jnp.bfloat16)
            wide = vector.astype(jnp.float32)
            squares = wide * wide
            vector_norm += squares[:8] + squares[8:]
            squares = recon * recon
            recon_norm += squares[:8] + squares[8:]
        vector_bias[:, pl.ds(n_at, LANES)] += vector_norm
        recon_bias[:, pl.ds(n_at, LANES)] += recon_norm
        return 0

    for load in loads[2:]:
        load.wait()

    done = 0
    for upto, z_arrivals, xy_arrivals in PLAN:
        with jax.named_scope("prepare"):
            lax.fori_loop(done, upto, prepare, 0, unroll=UNROLL)
        done = upto
        with jax.named_scope("relay"):
            for at in z_arrivals:
                block = arrived.at[at * PLANE, :, first_part]
                wait_bytes(block, near_first.at[at])
                send_xy(block, at)
            for group_at in xy_arrivals:
                block = arrived.at[group_at, :, second_part]
                wait_bytes(block, near_second.at[group_at])
                send_z(block, group_at)

    total = db * count
    lane = lax.broadcasted_iota(jnp.int32, (total, LANES), 1)
    row = lax.broadcasted_iota(jnp.int32, (total, LANES), 0)
    row_group = lax.rem(lax.div(row, count), PLANE)
    base = lax.rem(row, count)
    for group_at, (dx, dy) in enumerate(XY_STEPS):
        if dx:
            base = jnp.where(row_group == group_at, base + 16, base)
    lane_place[...] = lane - base
    out_row = lax.broadcasted_iota(jnp.int32, (NY * NZ, total), 0)
    from_row = lax.broadcasted_iota(jnp.int32, (NY * NZ, total), 1)
    from_group = lax.rem(lax.div(from_row, count), PLANE)
    from_place = lax.div(from_row, PLANE * count)
    for group_at, (dx, dy) in enumerate(XY_STEPS):
        if dy:
            from_place = jnp.where(from_group == group_at, from_place + dy * NZ, from_place)
    folder[...] = (from_place == out_row).astype(jnp.float32).astype(jnp.bfloat16)

    vector_row = jnp.sum(vector_bias[...], axis=0, keepdims=True) * (-SCALE / width)
    recon_row = jnp.sum(recon_bias[...], axis=0, keepdims=True) * (-SCALE / width)
    vector_bias[...] = jnp.broadcast_to(vector_row, vector_bias.shape)
    recon_bias[...] = jnp.broadcast_to(recon_row, recon_bias.shape)

    stack = 16 // count
    tile = 256
    half = half_steps * PLANE * count
    sums[...] = jnp.zeros_like(sums)

    def unpack(first, last):
        for index in range(first // stack, last // stack):
            blocks = [arrived[index * stack + i].astype(jnp.float32) for i in range(stack)]
            block = jnp.concatenate(blocks, axis=0)
            here = slice(index * 16, index * 16 + 16)
            own = block[:, :width]
            visiting[here, :] = own.astype(jnp.bfloat16)
            squares = own * own
            folded = squares[:, :LANES]
            for at in range(LANES, width, LANES):
                folded += squares[:, at : at + LANES]
            norm = jnp.sum(folded, axis=1, keepdims=True)
            bound = 1.9 + 0.6 * block[:, width:] / (LEVELS - 1)
            query_bias[here, :] = SCALE * bound - (SCALE / width) * norm

    def absorb(first):
        q_at = slice(first, first + half)

        def one(index, _):
            n_at = pl.ds(pl.multiple_of(index * tile, tile), tile)
            mine = visiting[q_at, :]
            cross = jnp.dot(mine, vectors[:, n_at], preferred_element_type=jnp.float32)
            coarse_cross = jnp.dot(mine, recons[:, n_at], preferred_element_type=jnp.float32)
            bias = query_bias[q_at, :]
            parts = [0.0, 0.0, 0.0]
            for at in range(0, tile, LANES):
                row_at = pl.ds(pl.multiple_of(index * tile + at, LANES), LANES)
                lanes = slice(at, at + LANES)
                exact = bias + (vector_bias[0:1, row_at] + cross[:, lanes] * (2 * SCALE / width))
                coarse = bias + (recon_bias[0:1, row_at] + coarse_cross[:, lanes] * (2 * SCALE / width))
                exact_hit = 1.0 + jnp.tanh(exact)
                coarse_hit = 1.0 + jnp.tanh(coarse)
                parts[0] += exact_hit
                parts[1] += coarse_hit
                parts[2] += exact_hit * coarse_hit
            for kind in range(3):
                sums[kind, q_at, :] += parts[kind]
            return 0

        lax.fori_loop(0, rows // tile, one, 0, unroll=ABSORB_UNROLL)

    def reduce_half(first):
        q_at = slice(first, first + half)
        place = lane_place[q_at, :]
        spread = jnp.zeros((half, LANES), jnp.float32)
        for kind in range(3):
            weight = 0.25 if kind == 2 else 0.5
            column = jnp.sum(sums[kind, q_at, :], axis=1, keepdims=True) * weight
            spread = jnp.where(place == count * kind, column, spread)
            spread = jnp.where(half_lane == 64 + kind, column, spread)
        spreads[q_at, :] = spread

    half_lane = lax.broadcasted_iota(jnp.int32, (half, LANES), 1)

    def wait_half(which):
        steps = half_steps - 1 + which
        first_span = pl.ds(which * half_steps * PLANE + 1, half_steps * (PLANE - 1))
        wait_bytes(arrived.at[first_span, :, first_part], far_first.at[which])
        start = half_steps if which else 1
        second_span = pl.ds(start * PLANE, steps * PLANE)
        wait_bytes(arrived.at[second_span, :, second_part], far_second.at[which])

    with jax.named_scope("wait_queries1"):
        wait_half(0)
    with jax.named_scope("unpack"):
        unpack(0, half_steps * PLANE)
    with jax.named_scope("absorb"):
        absorb(0)
    with jax.named_scope("wait_queries2"):
        wait_half(1)
    with jax.named_scope("unpack"):
        unpack(half_steps * PLANE, db)
    with jax.named_scope("absorb"):
        reduce_half(0)
        absorb(half)

    reduce_half(half)
    spread = spreads[...]
    overall = jnp.sum(spread, axis=0, keepdims=True)
    rest, folded = spread, 0.0
    for _ in range(3):
        piece = rest.astype(jnp.bfloat16)
        rest = rest - piece.astype(jnp.float32)
        folded += jnp.dot(folder[...], piece, preferred_element_type=jnp.float32)
    short_lane = lax.broadcasted_iota(jnp.int32, (NY * NZ, LANES), 1)
    folded = jnp.where(short_lane < 64, folded, overall)
    leaving[...] = folded.reshape(NY * NZ, 1, LANES)
    returned[0] = folded[0:1, :]

    for dy, at in ACROSS:
        place = dy * NZ + at
        start_copy(
            leaving.at[place],
            returned.at[place],
            hit_send,
            hit_recv,
            {"db": ahead(0, NY - dy, NZ - Z_STEPS[at])},
        )
    landing = returned.at[pl.ds(1, NY * NZ - 1)]
    with jax.named_scope("wait_hits"):
        wait_bytes(landing, hit_recv)
    mine = jnp.sum(returned[...], axis=0)
    own_sums[...] = mine
    for place, (dp, dx) in enumerate(sides):
        start_copy(own_sums, side_sums.at[place], side_send, side_recv, beside(dp, dx))
    with jax.named_scope("wait_totals"):
        wait_bytes(side_sums, side_recv)
    all_sums = mine + jnp.sum(side_sums[...], axis=0)
    partner = side_sums[sides.index((0, 1))]
    result_ref[0:1, :] = mine * (1.0 / database)
    result_ref[1:2, :] = partner * (1.0 / database)
    result_ref[2:3, :] = all_sums * (1.0 / (database * everyone))

    sent = arrived.at[pl.ds(1, db - 1)]
    wait_bytes(sent, query_send)
    wait_bytes(landing, hit_send)
    wait_bytes(side_sums, side_send)


UNROLL = 4
ABSORB_UNROLL = 4


def place_outputs(result_ref, hits_ref, totals_ref):
    count = hits_ref.shape[1]
    for kind in range(3):
        first = result_ref[0:1, kind * count : (kind + 1) * count]
        second = result_ref[1:2, 16 + kind * count : 16 + (kind + 1) * count]
        hits_ref[kind : kind + 1, :] = first + second
    totals_ref[...] = result_ref[2:3, 64:67]


def solution(mesh):
    db, pb = mesh.shape["db"], mesh.shape["pb"]

    def per_device(queries, residual, codes, codebook, ranks):
        count, width = queries.shape
        rows = residual.shape[0]
        subspaces, centroids, subdim = codebook.shape
        sizes = (db, pb, rows, width, rows * db, count * pb * db, subdim)
        total = db * count
        in_vmem = pl.BlockSpec(memory_space=pltpu.VMEM)
        anywhere = pl.BlockSpec(memory_space=pl.ANY)
        dma = pltpu.SemaphoreType.DMA
        result = pl.pallas_call(
            lambda *refs: kernel_body(sizes, *refs),
            out_shape=pltpu.VMEM((8, LANES), jnp.float32),
            in_specs=[anywhere] * 5,
            out_specs=in_vmem,
            scratch_shapes=[
                pltpu.SMEM((count,), jnp.int32),
                pltpu.VMEM((count, width), jnp.bfloat16),
                pltpu.VMEM((count, width + LANES), jnp.bfloat16),
                pltpu.VMEM((db, count, width + LANES), jnp.bfloat16),
                pltpu.VMEM((subspaces, subdim, centroids), jnp.float32),
                pltpu.VMEM((subspaces, rows), jnp.int32),
                pltpu.VMEM((rows, width), jnp.bfloat16),
                pltpu.VMEM((width, rows), jnp.bfloat16),
                pltpu.VMEM((width, rows), jnp.bfloat16),
                pltpu.VMEM((8, rows), jnp.float32),
                pltpu.VMEM((8, rows), jnp.float32),
                pltpu.VMEM((total, width), jnp.bfloat16),
                pltpu.VMEM((total, LANES), jnp.float32),
                pltpu.VMEM((3, total, LANES), jnp.float32),
                pltpu.VMEM((total, LANES), jnp.int32),
                pltpu.VMEM((total, LANES), jnp.float32),
                pltpu.VMEM((NY * NZ, total), jnp.bfloat16),
                pltpu.VMEM((NY * NZ, 1, LANES), jnp.float32),
                pltpu.VMEM((NY * NZ, 1, LANES), jnp.float32),
                pltpu.VMEM((1, LANES), jnp.float32),
                pltpu.VMEM((pb * NX - 1, 1, LANES), jnp.float32),
                dma((5,)),
                dma,
                dma((NZ,)),
                dma((PLANE,)),
                dma((2,)),
                dma((2,)),
                dma,
                dma,
                dma,
                dma,
            ],
            compiler_params=pltpu.CompilerParams(
                collective_id=0, has_side_effects=True, vmem_limit_bytes=60 * 1024 * 1024
            ),
            name="recall",
        )(ranks, queries, residual, codes.T, jnp.transpose(codebook, (0, 2, 1)))
        hits, totals = pl.pallas_call(
            place_outputs,
            out_shape=(
                jax.ShapeDtypeStruct((3, count), jnp.float32),
                jax.ShapeDtypeStruct((1, 3), jnp.float32),
            ),
            in_specs=[in_vmem],
            name="place",
        )(pltpu.with_memory_space_constraint(result, pltpu.VMEM))
        return hits, totals.reshape(3)

    return jax.shard_map(
        per_device,
        mesh=mesh,
        in_specs=(P(("pb", "db"), None), P("db", None), P("db", None), P(), P(("pb", "db"))),
        out_specs=(P(None, ("pb", "db")), P()),
        check_vma=False,
    )
```

```python
import jax
import jax.numpy as jnp
from jax import lax
from jax.experimental import pallas as pl
from jax.experimental.pallas import tpu as pltpu
from jax.sharding import PartitionSpec as P

LEVELS = 64
SCALE = 25.0
LANES = 128
MESH = pl.DeviceIdType.MESH
NX, NY, NZ = 2, 4, 8
PLANE = NX * NY
FIRST_COLUMNS = 768
Z_STEPS = (0, 1, 7, 2, 6, 3, 5, 4)
XY_STEPS = ((0, 0), (0, 1), (0, 3), (1, 0), (1, 1), (1, 3), (0, 2), (1, 2))


def ring(step, length):
    return min(step, length - step)


ACROSS = sorted(
    ((dy, at) for dy in range(NY) for at in range(NZ) if dy + at),
    key=lambda step: -ring(step[0], NY) - ring(Z_STEPS[step[1]], NZ),
)
PLAN = ((16, (1, 2), (1, 2, 3)), (20, (3, 4), (4, 5, 6)), (24, (5, 6), (7,)), (28, (7,), ()), (64, (), ()))


def lane_gather(rows, index):
    numbers = lax.GatherDimensionNumbers(
        offset_dims=(),
        collapsed_slice_dims=(1,),
        start_index_map=(1,),
        operand_batching_dims=(0,),
        start_indices_batching_dims=(0,),
    )
    return lax.gather(
        rows,
        index[:, :, None],
        dimension_numbers=numbers,
        slice_sizes=(1, 1),
        mode=lax.GatherScatterMode.PROMISE_IN_BOUNDS,
    )


def start_copy(source, target, send_sem, recv_sem, device):
    pltpu.make_async_remote_copy(
        src_ref=source,
        dst_ref=target,
        send_sem=send_sem,
        recv_sem=recv_sem,
        device_id=device,
        device_id_type=MESH,
    ).start()


def wait_bytes(block, sem):
    pltpu.make_async_copy(block, block, sem).wait()


def kernel_body(
    sizes,
    ranks_ref,
    queries_ref,
    residual_ref,
    codes_ref,
    codebook_ref,
    result_ref,
    own_ranks,
    own_queries,
    message,
    arrived,
    table,
    codes,
    residual,
    vectors,
    recons,
    vector_bias,
    recon_bias,
    visiting,
    query_bias,
    sums,
    lane_place,
    spreads,
    folder,
    leaving,
    returned,
    own_sums,
    side_sums,
    local_sems,
    query_send,
    near_first,
    near_second,
    far_first,
    far_second,
    hit_send,
    hit_recv,
    side_send,
    side_recv,
):
    db, pb, rows, width, database, everyone, subdim = sizes
    count = own_queries.shape[0]
    me = lax.axis_index("db")
    my_pb = lax.axis_index("pb")

    loads = [
        pltpu.make_async_copy(ranks_ref, own_ranks, local_sems.at[4]),
        pltpu.make_async_copy(queries_ref, own_queries, local_sems.at[3]),
        pltpu.make_async_copy(codebook_ref, table, local_sems.at[0]),
        pltpu.make_async_copy(codes_ref, codes, local_sems.at[1]),
        pltpu.make_async_copy(residual_ref, residual, local_sems.at[2]),
    ]

    my_x, my_y, my_z = lax.div(me, NY * NZ), lax.rem(lax.div(me, NZ), NY), lax.rem(me, NZ)

    def ahead(dx, dy, dz):
        x, y, z = lax.rem(my_x + dx, NX), lax.rem(my_y + dy, NY), lax.rem(my_z + dz, NZ)
        return (x * NY + y) * NZ + z

    def beside(dp, dx):
        return {"pb": lax.rem(my_pb + dp, pb), "db": ahead(dx, 0, 0)}

    sides = [(dp, dx) for dp in range(pb) for dx in range(NX) if dp + dx]

    barrier = pltpu.get_barrier_semaphore()
    greeted = [{"db": ahead(0, 0, dz)} for dz in Z_STEPS[:0:-1]]
    greeted += [{"db": ahead(dx, dy, 0)} for dx, dy in XY_STEPS[:0:-1]]
    greeted += [beside(dp, dx) for dp, dx in sides if dp]
    for load in loads[:2]:
        load.start()
    for device in greeted:
        pl.semaphore_signal(barrier, inc=1, device_id=device, device_id_type=MESH)
    for load in loads[2:]:
        load.start()

    row_ids = lax.broadcasted_iota(jnp.int32, (count, LANES), 0)
    rank_block = jnp.zeros((count, LANES), jnp.float32)
    loads[0].wait()
    for row in range(count):
        rank_block = jnp.where(row_ids == row, own_ranks[row].astype(jnp.float32), rank_block)
    message[:, width:] = rank_block.astype(jnp.bfloat16)
    loads[1].wait()
    message[:, :width] = own_queries[...]
    arrived[0] = message[...]
    vector_bias[...] = jnp.zeros_like(vector_bias)
    recon_bias[...] = jnp.zeros_like(recon_bias)

    with jax.named_scope("wait_barrier"):
        pl.semaphore_wait(barrier, len(greeted))

    first_part, second_part = pl.ds(0, FIRST_COLUMNS), pl.ds(FIRST_COLUMNS, width + LANES - FIRST_COLUMNS)
    half_steps = NZ // 2

    def send_xy(source, at):
        for group_at in range(PLANE - 1, 0, -1):
            dx, dy = XY_STEPS[group_at]
            start_copy(
                source,
                arrived.at[at * PLANE + group_at, :, first_part],
                query_send,
                far_first.at[at // half_steps],
                {"db": ahead(dx, dy, 0)},
            )

    def send_z(source, group_at):
        for at in range(NZ - 1, 0, -1):
            start_copy(
                source,
                arrived.at[at * PLANE + group_at, :, second_part],
                query_send,
                far_second.at[at // half_steps],
                {"db": ahead(0, 0, Z_STEPS[at])},
            )

    for at in range(1, NZ):
        start_copy(
            message.at[:, first_part],
            arrived.at[at * PLANE, :, first_part],
            query_send,
            near_first.at[at],
            {"db": ahead(0, 0, Z_STEPS[at])},
        )
    for group_at in range(1, PLANE):
        dx, dy = XY_STEPS[group_at]
        start_copy(
            message.at[:, second_part],
            arrived.at[group_at, :, second_part],
            query_send,
            near_second.at[group_at],
            {"db": ahead(dx, dy, 0)},
        )
    send_xy(message.at[:, first_part], 0)
    send_z(message.at[:, second_part], 0)

    group = LANES // subdim
    parts = width // LANES

    def prepare(index, _):
        at, part = lax.div(index, parts), lax.rem(index, parts)
        n_at = pl.multiple_of(at * LANES, LANES)
        d_at = pl.multiple_of(part * LANES, LANES)
        extra = residual[pl.ds(n_at, LANES), pl.ds(d_at, LANES)].T
        chosen = codes[pl.ds(pl.multiple_of(part * group, group), group), pl.ds(n_at, LANES)]
        vector_norm = jnp.zeros((8, LANES), jnp.float32)
        recon_norm = jnp.zeros((8, LANES), jnp.float32)
        for inner in range(group):
            pick = jnp.broadcast_to(chosen[inner : inner + 1, :], (subdim, LANES))
            low_pick = pick & (LANES - 1)
            entries = table[part * group + inner]
            below = lane_gather(entries[:, :LANES], low_pick)
            above = lane_gather(entries[:, LANES:], low_pick)
            recon = jnp.where(pick >= LANES, above, below)
            addend = extra[inner * subdim : (inner + 1) * subdim, :].astype(jnp.float32)
            vector = (recon + addend).astype(jnp.bfloat16)
            here = pl.ds(pl.multiple_of(d_at + inner * subdim, subdim), subdim)
            vectors[here, pl.ds(n_at, LANES)] = vector
            recons[here, pl.ds(n_at, LANES)] = recon.astype(jnp.bfloat16)
            wide = vector.astype(jnp.float32)
            squares = wide * wide
            vector_norm += squares[:8] + squares[8:]
            squares = recon * recon
            recon_norm += squares[:8] + squares[8:]
        vector_bias[:, pl.ds(n_at, LANES)] += vector_norm
        recon_bias[:, pl.ds(n_at, LANES)] += recon_norm
        return 0

    for load in loads[2:]:
        load.wait()

    done = 0
    for upto, z_arrivals, xy_arrivals in PLAN:
        with jax.named_scope("prepare"):
            lax.fori_loop(done, upto, prepare, 0, unroll=UNROLL)
        done = upto
        with jax.named_scope("relay"):
            for at in z_arrivals:
                block = arrived.at[at * PLANE, :, first_part]
                wait_bytes(block, near_first.at[at])
                send_xy(block, at)
            for group_at in xy_arrivals:
                block = arrived.at[group_at, :, second_part]
                wait_bytes(block, near_second.at[group_at])
                send_z(block, group_at)

    total = db * count
    lane = lax.broadcasted_iota(jnp.int32, (total, LANES), 1)
    row = lax.broadcasted_iota(jnp.int32, (total, LANES), 0)
    row_group = lax.rem(lax.div(row, count), PLANE)
    base = lax.rem(row, count)
    for group_at, (dx, dy) in enumerate(XY_STEPS):
        if dx:
            base = jnp.where(row_group == group_at, base + 16, base)
    lane_place[...] = lane - base
    out_row = lax.broadcasted_iota(jnp.int32, (NY * NZ, total), 0)
    from_row = lax.broadcasted_iota(jnp.int32, (NY * NZ, total), 1)
    from_group = lax.rem(lax.div(from_row, count), PLANE)
    from_place = lax.div(from_row, PLANE * count)
    for group_at, (dx, dy) in enumerate(XY_STEPS):
        if dy:
            from_place = jnp.where(from_group == group_at, from_place + dy * NZ, from_place)
    folder[...] = (from_place == out_row).astype(jnp.float32).astype(jnp.bfloat16)

    vector_row = jnp.sum(vector_bias[...], axis=0, keepdims=True) * (-SCALE / width)
    recon_row = jnp.sum(recon_bias[...], axis=0, keepdims=True) * (-SCALE / width)
    vector_bias[...] = jnp.broadcast_to(vector_row, vector_bias.shape)
    recon_bias[...] = jnp.broadcast_to(recon_row, recon_bias.shape)

    stack = 16 // count
    tile = 256
    half = half_steps * PLANE * count
    sums[...] = jnp.zeros_like(sums)

    def unpack(first, last):
        for index in range(first // stack, last // stack):
            blocks = [arrived[index * stack + i].astype(jnp.float32) for i in range(stack)]
            block = jnp.concatenate(blocks, axis=0)
            here = slice(index * 16, index * 16 + 16)
            own = block[:, :width]
            visiting[here, :] = own.astype(jnp.bfloat16)
            squares = own * own
            folded = squares[:, :LANES]
            for at in range(LANES, width, LANES):
                folded += squares[:, at : at + LANES]
            norm = jnp.sum(folded, axis=1, keepdims=True)
            bound = 1.9 + 0.6 * block[:, width:] / (LEVELS - 1)
            query_bias[here, :] = SCALE * bound - (SCALE / width) * norm

    def absorb(first):
        q_at = slice(first, first + half)

        def one(index, _):
            n_at = pl.ds(pl.multiple_of(index * tile, tile), tile)
            mine = visiting[q_at, :]
            cross = jnp.dot(mine, vectors[:, n_at], preferred_element_type=jnp.float32)
            coarse_cross = jnp.dot(mine, recons[:, n_at], preferred_element_type=jnp.float32)
            bias = query_bias[q_at, :]
            parts = [0.0, 0.0, 0.0]
            for at in range(0, tile, LANES):
                row_at = pl.ds(pl.multiple_of(index * tile + at, LANES), LANES)
                lanes = slice(at, at + LANES)
                exact = bias + (vector_bias[0:1, row_at] + cross[:, lanes] * (2 * SCALE / width))
                coarse = bias + (recon_bias[0:1, row_at] + coarse_cross[:, lanes] * (2 * SCALE / width))
                exact_hit = 1.0 + jnp.tanh(exact)
                coarse_hit = 1.0 + jnp.tanh(coarse)
                parts[0] += exact_hit
                parts[1] += coarse_hit
                parts[2] += exact_hit * coarse_hit
            for kind in range(3):
                sums[kind, q_at, :] += parts[kind]
            return 0

        lax.fori_loop(0, rows // tile, one, 0, unroll=ABSORB_UNROLL)

    def reduce_half(first):
        q_at = slice(first, first + half)
        place = lane_place[q_at, :]
        spread = jnp.zeros((half, LANES), jnp.float32)
        for kind in range(3):
            weight = 0.25 if kind == 2 else 0.5
            column = jnp.sum(sums[kind, q_at, :], axis=1, keepdims=True) * weight
            spread = jnp.where(place == count * kind, column, spread)
            spread = jnp.where(half_lane == 64 + kind, column, spread)
        spreads[q_at, :] = spread

    half_lane = lax.broadcasted_iota(jnp.int32, (half, LANES), 1)

    def wait_half(which):
        steps = half_steps - 1 + which
        first_span = pl.ds(which * half_steps * PLANE + 1, half_steps * (PLANE - 1))
        wait_bytes(arrived.at[first_span, :, first_part], far_first.at[which])
        start = half_steps if which else 1
        second_span = pl.ds(start * PLANE, steps * PLANE)
        wait_bytes(arrived.at[second_span, :, second_part], far_second.at[which])

    with jax.named_scope("wait_queries1"):
        wait_half(0)
    with jax.named_scope("unpack"):
        unpack(0, half_steps * PLANE)
    with jax.named_scope("absorb"):
        absorb(0)
    with jax.named_scope("wait_queries2"):
        wait_half(1)
    with jax.named_scope("unpack"):
        unpack(half_steps * PLANE, db)
    with jax.named_scope("absorb"):
        reduce_half(0)
        absorb(half)

    reduce_half(half)
    spread = spreads[...]
    overall = jnp.sum(spread, axis=0, keepdims=True)
    rest, folded = spread, 0.0
    for _ in range(3):
        piece = rest.astype(jnp.bfloat16)
        rest = rest - piece.astype(jnp.float32)
        folded += jnp.dot(folder[...], piece, preferred_element_type=jnp.float32)
    short_lane = lax.broadcasted_iota(jnp.int32, (NY * NZ, LANES), 1)
    folded = jnp.where(short_lane < 64, folded, overall)
    leaving[...] = folded.reshape(NY * NZ, 1, LANES)
    returned[0] = folded[0:1, :]

    for dy, at in ACROSS:
        place = dy * NZ + at
        start_copy(
            leaving.at[place],
            returned.at[place],
            hit_send,
            hit_recv,
            {"db": ahead(0, NY - dy, NZ - Z_STEPS[at])},
        )
    landing = returned.at[pl.ds(1, NY * NZ - 1)]
    with jax.named_scope("wait_hits"):
        wait_bytes(landing, hit_recv)
    mine = jnp.sum(returned[...], axis=0)
    own_sums[...] = mine
    for place, (dp, dx) in enumerate(sides):
        start_copy(own_sums, side_sums.at[place], side_send, side_recv, beside(dp, dx))
    with jax.named_scope("wait_totals"):
        wait_bytes(side_sums, side_recv)
    all_sums = mine + jnp.sum(side_sums[...], axis=0)
    partner = side_sums[sides.index((0, 1))]
    result_ref[0:1, :] = mine * (1.0 / database)
    result_ref[1:2, :] = partner * (1.0 / database)
    result_ref[2:3, :] = all_sums * (1.0 / (database * everyone))

    sent = arrived.at[pl.ds(1, db - 1)]
    wait_bytes(sent, query_send)
    wait_bytes(landing, hit_send)
    wait_bytes(side_sums, side_send)


UNROLL = 4
ABSORB_UNROLL = 4


def place_outputs(result_ref, hits_ref, totals_ref):
    count = hits_ref.shape[1]
    for kind in range(3):
        first = result_ref[0:1, kind * count : (kind + 1) * count]
        second = result_ref[1:2, 16 + kind * count : 16 + (kind + 1) * count]
        hits_ref[kind : kind + 1, :] = first + second
    totals_ref[...] = result_ref[2:3, 64:67]


def solution(mesh):
    db, pb = mesh.shape["db"], mesh.shape["pb"]

    def per_device(queries, residual, codes, codebook, ranks):
        count, width = queries.shape
        rows = residual.shape[0]
        subspaces, centroids, subdim = codebook.shape
        sizes = (db, pb, rows, width, rows * db, count * pb * db, subdim)
        total = db * count
        in_vmem = pl.BlockSpec(memory_space=pltpu.VMEM)
        anywhere = pl.BlockSpec(memory_space=pl.ANY)
        dma = pltpu.SemaphoreType.DMA
        result = pl.pallas_call(
            lambda *refs: kernel_body(sizes, *refs),
            out_shape=pltpu.VMEM((8, LANES), jnp.float32),
            in_specs=[anywhere] * 5,
            out_specs=in_vmem,
            scratch_shapes=[
                pltpu.SMEM((count,), jnp.int32),
                pltpu.VMEM((count, width), jnp.bfloat16),
                pltpu.VMEM((count, width + LANES), jnp.bfloat16),
                pltpu.VMEM((db, count, width + LANES), jnp.bfloat16),
                pltpu.VMEM((subspaces, subdim, centroids), jnp.float32),
                pltpu.VMEM((subspaces, rows), jnp.int32),
                pltpu.VMEM((rows, width), jnp.bfloat16),
                pltpu.VMEM((width, rows), jnp.bfloat16),
                pltpu.VMEM((width, rows), jnp.bfloat16),
                pltpu.VMEM((8, rows), jnp.float32),
                pltpu.VMEM((8, rows), jnp.float32),
                pltpu.VMEM((total, width), jnp.bfloat16),
                pltpu.VMEM((total, LANES), jnp.float32),
                pltpu.VMEM((3, total, LANES), jnp.float32),
                pltpu.VMEM((total, LANES), jnp.int32),
                pltpu.VMEM((total, LANES), jnp.float32),
                pltpu.VMEM((NY * NZ, total), jnp.bfloat16),
                pltpu.VMEM((NY * NZ, 1, LANES), jnp.float32),
                pltpu.VMEM((NY * NZ, 1, LANES), jnp.float32),
                pltpu.VMEM((1, LANES), jnp.float32),
                pltpu.VMEM((pb * NX - 1, 1, LANES), jnp.float32),
                dma((5,)),
                dma,
                dma((NZ,)),
                dma((PLANE,)),
                dma((2,)),
                dma((2,)),
                dma,
                dma,
                dma,
                dma,
            ],
            compiler_params=pltpu.CompilerParams(
                collective_id=0, has_side_effects=True, vmem_limit_bytes=60 * 1024 * 1024
            ),
            name="recall",
        )(ranks, queries, residual, codes.T, jnp.transpose(codebook, (0, 2, 1)))
        hits, totals = pl.pallas_call(
            place_outputs,
            out_shape=(
                jax.ShapeDtypeStruct((3, count), jnp.float32),
                jax.ShapeDtypeStruct((1, 3), jnp.float32),
            ),
            in_specs=[in_vmem],
            name="place",
        )(pltpu.with_memory_space_constraint(result, pltpu.VMEM))
        return hits, totals.reshape(3)

    return jax.shard_map(
        per_device,
        mesh=mesh,
        in_specs=(P(("pb", "db"), None), P("db", None), P("db", None), P(), P(("pb", "db"))),
        out_specs=(P(None, ("pb", "db")), P()),
        check_vma=False,
    )
```

```python
import jax
import jax.numpy as jnp
from jax import lax
from jax.experimental import pallas as pl
from jax.experimental.pallas import tpu as pltpu
from jax.sharding import PartitionSpec as P

LEVELS = 64
SCALE = 25.0
LANES = 128
MESH = pl.DeviceIdType.MESH
NX, NY, NZ = 2, 4, 8
PLANE = NX * NY
FIRST_COLUMNS = 768
Z_STEPS = (0, 1, 7, 2, 6, 3, 5, 4)
XY_STEPS = ((0, 0), (0, 1), (0, 3), (1, 0), (1, 1), (1, 3), (0, 2), (1, 2))


def ring(step, length):
    return min(step, length - step)


ACROSS = sorted(
    ((dy, at) for dy in range(NY) for at in range(NZ) if dy + at),
    key=lambda step: -ring(step[0], NY) - ring(Z_STEPS[step[1]], NZ),
)
PLAN = ((16, (1, 2), (1, 2, 3)), (20, (3, 4), (4, 5, 6, 7)), (28, (5, 6), ()), (32, (7,), ()), (64, (), ()))


def lane_gather(rows, index):
    numbers = lax.GatherDimensionNumbers(
        offset_dims=(),
        collapsed_slice_dims=(1,),
        start_index_map=(1,),
        operand_batching_dims=(0,),
        start_indices_batching_dims=(0,),
    )
    return lax.gather(
        rows,
        index[:, :, None],
        dimension_numbers=numbers,
        slice_sizes=(1, 1),
        mode=lax.GatherScatterMode.PROMISE_IN_BOUNDS,
    )


def start_copy(source, target, send_sem, recv_sem, device):
    pltpu.make_async_remote_copy(
        src_ref=source,
        dst_ref=target,
        send_sem=send_sem,
        recv_sem=recv_sem,
        device_id=device,
        device_id_type=MESH,
    ).start()


def wait_bytes(block, sem):
    pltpu.make_async_copy(block, block, sem).wait()


def kernel_body(
    sizes,
    ranks_ref,
    queries_ref,
    residual_ref,
    codes_ref,
    codebook_ref,
    result_ref,
    own_ranks,
    own_queries,
    message,
    arrived,
    table,
    codes,
    residual,
    vectors,
    recons,
    vector_bias,
    recon_bias,
    visiting,
    query_bias,
    sums,
    lane_place,
    spreads,
    folder,
    leaving,
    returned,
    own_sums,
    side_sums,
    local_sems,
    query_send,
    near_first,
    near_second,
    far_first,
    far_second,
    hit_send,
    hit_recv,
    side_send,
    side_recv,
):
    db, pb, rows, width, database, everyone, subdim = sizes
    count = own_queries.shape[0]
    me = lax.axis_index("db")
    my_pb = lax.axis_index("pb")

    loads = [
        pltpu.make_async_copy(ranks_ref, own_ranks, local_sems.at[4]),
        pltpu.make_async_copy(queries_ref, own_queries, local_sems.at[3]),
        pltpu.make_async_copy(codebook_ref, table, local_sems.at[0]),
        pltpu.make_async_copy(codes_ref, codes, local_sems.at[1]),
        pltpu.make_async_copy(residual_ref, residual, local_sems.at[2]),
    ]

    my_x, my_y, my_z = lax.div(me, NY * NZ), lax.rem(lax.div(me, NZ), NY), lax.rem(me, NZ)

    def ahead(dx, dy, dz):
        x, y, z = lax.rem(my_x + dx, NX), lax.rem(my_y + dy, NY), lax.rem(my_z + dz, NZ)
        return (x * NY + y) * NZ + z

    def beside(dp, dx):
        return {"pb": lax.rem(my_pb + dp, pb), "db": ahead(dx, 0, 0)}

    sides = [(dp, dx) for dp in range(pb) for dx in range(NX) if dp + dx]

    barrier = pltpu.get_barrier_semaphore()
    greeted = [{"db": ahead(0, 0, dz)} for dz in Z_STEPS[:0:-1]]
    greeted += [{"db": ahead(dx, dy, 0)} for dx, dy in XY_STEPS[:0:-1]]
    greeted += [beside(dp, dx) for dp, dx in sides if dp]
    for load in loads[:2]:
        load.start()
    for device in greeted:
        pl.semaphore_signal(barrier, inc=1, device_id=device, device_id_type=MESH)
    for load in loads[2:]:
        load.start()

    row_ids = lax.broadcasted_iota(jnp.int32, (count, LANES), 0)
    rank_block = jnp.zeros((count, LANES), jnp.float32)
    loads[0].wait()
    for row in range(count):
        rank_block = jnp.where(row_ids == row, own_ranks[row].astype(jnp.float32), rank_block)
    message[:, width:] = rank_block.astype(jnp.bfloat16)
    loads[1].wait()
    message[:, :width] = own_queries[...]
    arrived[0] = message[...]
    vector_bias[...] = jnp.zeros_like(vector_bias)
    recon_bias[...] = jnp.zeros_like(recon_bias)

    with jax.named_scope("wait_barrier"):
        pl.semaphore_wait(barrier, len(greeted))

    first_part, second_part = pl.ds(0, FIRST_COLUMNS), pl.ds(FIRST_COLUMNS, width + LANES - FIRST_COLUMNS)
    half_steps = NZ // 2

    def send_xy(source, at):
        for group_at in range(PLANE - 1, 0, -1):
            dx, dy = XY_STEPS[group_at]
            start_copy(
                source,
                arrived.at[at * PLANE + group_at, :, first_part],
                query_send,
                far_first.at[at // half_steps],
                {"db": ahead(dx, dy, 0)},
            )

    def send_z(source, group_at):
        for at in range(NZ - 1, 0, -1):
            start_copy(
                source,
                arrived.at[at * PLANE + group_at, :, second_part],
                query_send,
                far_second.at[at // half_steps],
                {"db": ahead(0, 0, Z_STEPS[at])},
            )

    for at in range(1, NZ):
        start_copy(
            message.at[:, first_part],
            arrived.at[at * PLANE, :, first_part],
            query_send,
            near_first.at[at],
            {"db": ahead(0, 0, Z_STEPS[at])},
        )
    for group_at in range(1, PLANE):
        dx, dy = XY_STEPS[group_at]
        start_copy(
            message.at[:, second_part],
            arrived.at[group_at, :, second_part],
            query_send,
            near_second.at[group_at],
            {"db": ahead(dx, dy, 0)},
        )
    send_xy(message.at[:, first_part], 0)
    send_z(message.at[:, second_part], 0)

    group = LANES // subdim
    parts = width // LANES

    def prepare(index, _):
        at, part = lax.div(index, parts), lax.rem(index, parts)
        n_at = pl.multiple_of(at * LANES, LANES)
        d_at = pl.multiple_of(part * LANES, LANES)
        extra = residual[pl.ds(n_at, LANES), pl.ds(d_at, LANES)].T
        chosen = codes[pl.ds(pl.multiple_of(part * group, group), group), pl.ds(n_at, LANES)]
        vector_norm = jnp.zeros((8, LANES), jnp.float32)
        recon_norm = jnp.zeros((8, LANES), jnp.float32)
        for inner in range(group):
            pick = jnp.broadcast_to(chosen[inner : inner + 1, :], (subdim, LANES))
            low_pick = pick & (LANES - 1)
            entries = table[part * group + inner]
            below = lane_gather(entries[:, :LANES], low_pick)
            above = lane_gather(entries[:, LANES:], low_pick)
            recon = jnp.where(pick >= LANES, above, below)
            addend = extra[inner * subdim : (inner + 1) * subdim, :].astype(jnp.float32)
            vector = (recon + addend).astype(jnp.bfloat16)
            here = pl.ds(pl.multiple_of(d_at + inner * subdim, subdim), subdim)
            vectors[here, pl.ds(n_at, LANES)] = vector
            recons[here, pl.ds(n_at, LANES)] = recon.astype(jnp.bfloat16)
            wide = vector.astype(jnp.float32)
            squares = wide * wide
            vector_norm += squares[:8] + squares[8:]
            squares = recon * recon
            recon_norm += squares[:8] + squares[8:]
        vector_bias[:, pl.ds(n_at, LANES)] += vector_norm
        recon_bias[:, pl.ds(n_at, LANES)] += recon_norm
        return 0

    for load in loads[2:]:
        load.wait()

    done = 0
    for upto, z_arrivals, xy_arrivals in PLAN:
        with jax.named_scope("prepare"):
            lax.fori_loop(done, upto, prepare, 0, unroll=UNROLL)
        done = upto
        with jax.named_scope("relay"):
            for at in z_arrivals:
                block = arrived.at[at * PLANE, :, first_part]
                wait_bytes(block, near_first.at[at])
                send_xy(block, at)
            for group_at in xy_arrivals:
                block = arrived.at[group_at, :, second_part]
                wait_bytes(block, near_second.at[group_at])
                send_z(block, group_at)

    total = db * count
    lane = lax.broadcasted_iota(jnp.int32, (total, LANES), 1)
    row = lax.broadcasted_iota(jnp.int32, (total, LANES), 0)
    row_group = lax.rem(lax.div(row, count), PLANE)
    base = lax.rem(row, count)
    for group_at, (dx, dy) in enumerate(XY_STEPS):
        if dx:
            base = jnp.where(row_group == group_at, base + 16, base)
    lane_place[...] = lane - base
    out_row = lax.broadcasted_iota(jnp.int32, (NY * NZ, total), 0)
    from_row = lax.broadcasted_iota(jnp.int32, (NY * NZ, total), 1)
    from_group = lax.rem(lax.div(from_row, count), PLANE)
    from_place = lax.div(from_row, PLANE * count)
    for group_at, (dx, dy) in enumerate(XY_STEPS):
        if dy:
            from_place = jnp.where(from_group == group_at, from_place + dy * NZ, from_place)
    folder[...] = (from_place == out_row).astype(jnp.float32).astype(jnp.bfloat16)

    vector_row = jnp.sum(vector_bias[...], axis=0, keepdims=True) * (-SCALE / width)
    recon_row = jnp.sum(recon_bias[...], axis=0, keepdims=True) * (-SCALE / width)
    vector_bias[...] = jnp.broadcast_to(vector_row, vector_bias.shape)
    recon_bias[...] = jnp.broadcast_to(recon_row, recon_bias.shape)

    stack = 16 // count
    tile = 256
    half = half_steps * PLANE * count
    sums[...] = jnp.zeros_like(sums)

    def unpack(first, last):
        for index in range(first // stack, last // stack):
            blocks = [arrived[index * stack + i].astype(jnp.float32) for i in range(stack)]
            block = jnp.concatenate(blocks, axis=0)
            here = slice(index * 16, index * 16 + 16)
            own = block[:, :width]
            visiting[here, :] = own.astype(jnp.bfloat16)
            squares = own * own
            folded = squares[:, :LANES]
            for at in range(LANES, width, LANES):
                folded += squares[:, at : at + LANES]
            norm = jnp.sum(folded, axis=1, keepdims=True)
            bound = 1.9 + 0.6 * block[:, width:] / (LEVELS - 1)
            query_bias[here, :] = SCALE * bound - (SCALE / width) * norm

    def absorb(first):
        q_at = slice(first, first + half)

        def one(index, _):
            n_at = pl.ds(pl.multiple_of(index * tile, tile), tile)
            mine = visiting[q_at, :]
            cross = jnp.dot(mine, vectors[:, n_at], preferred_element_type=jnp.float32)
            coarse_cross = jnp.dot(mine, recons[:, n_at], preferred_element_type=jnp.float32)
            bias = query_bias[q_at, :]
            parts = [0.0, 0.0, 0.0]
            for at in range(0, tile, LANES):
                row_at = pl.ds(pl.multiple_of(index * tile + at, LANES), LANES)
                lanes = slice(at, at + LANES)
                exact = bias + (vector_bias[0:1, row_at] + cross[:, lanes] * (2 * SCALE / width))
                coarse = bias + (recon_bias[0:1, row_at] + coarse_cross[:, lanes] * (2 * SCALE / width))
                exact_hit = 1.0 + jnp.tanh(exact)
                coarse_hit = 1.0 + jnp.tanh(coarse)
                parts[0] += exact_hit
                parts[1] += coarse_hit
                parts[2] += exact_hit * coarse_hit
            for kind in range(3):
                sums[kind, q_at, :] += parts[kind]
            return 0

        lax.fori_loop(0, rows // tile, one, 0, unroll=ABSORB_UNROLL)

    def reduce_half(first):
        q_at = slice(first, first + half)
        place = lane_place[q_at, :]
        spread = jnp.zeros((half, LANES), jnp.float32)
        for kind in range(3):
            weight = 0.25 if kind == 2 else 0.5
            column = jnp.sum(sums[kind, q_at, :], axis=1, keepdims=True) * weight
            spread = jnp.where(place == count * kind, column, spread)
            spread = jnp.where(half_lane == 64 + kind, column, spread)
        spreads[q_at, :] = spread

    half_lane = lax.broadcasted_iota(jnp.int32, (half, LANES), 1)

    def wait_half(which):
        steps = half_steps - 1 + which
        first_span = pl.ds(which * half_steps * PLANE + 1, half_steps * (PLANE - 1))
        wait_bytes(arrived.at[first_span, :, first_part], far_first.at[which])
        start = half_steps if which else 1
        second_span = pl.ds(start * PLANE, steps * PLANE)
        wait_bytes(arrived.at[second_span, :, second_part], far_second.at[which])

    with jax.named_scope("wait_queries1"):
        wait_half(0)
    with jax.named_scope("unpack"):
        unpack(0, half_steps * PLANE)
    with jax.named_scope("absorb"):
        absorb(0)
    with jax.named_scope("wait_queries2"):
        wait_half(1)
    with jax.named_scope("unpack"):
        unpack(half_steps * PLANE, db)
    with jax.named_scope("absorb"):
        reduce_half(0)
        absorb(half)

    reduce_half(half)
    spread = spreads[...]
    overall = jnp.sum(spread, axis=0, keepdims=True)
    rest, folded = spread, 0.0
    for _ in range(3):
        piece = rest.astype(jnp.bfloat16)
        rest = rest - piece.astype(jnp.float32)
        folded += jnp.dot(folder[...], piece, preferred_element_type=jnp.float32)
    short_lane = lax.broadcasted_iota(jnp.int32, (NY * NZ, LANES), 1)
    folded = jnp.where(short_lane < 64, folded, overall)
    leaving[...] = folded.reshape(NY * NZ, 1, LANES)
    returned[0] = folded[0:1, :]

    for dy, at in ACROSS:
        place = dy * NZ + at
        start_copy(
            leaving.at[place],
            returned.at[place],
            hit_send,
            hit_recv,
            {"db": ahead(0, NY - dy, NZ - Z_STEPS[at])},
        )
    landing = returned.at[pl.ds(1, NY * NZ - 1)]
    with jax.named_scope("wait_hits"):
        wait_bytes(landing, hit_recv)
    mine = jnp.sum(returned[...], axis=0)
    own_sums[...] = mine
    for place, (dp, dx) in enumerate(sides):
        start_copy(own_sums, side_sums.at[place], side_send, side_recv, beside(dp, dx))
    with jax.named_scope("wait_totals"):
        wait_bytes(side_sums, side_recv)
    all_sums = mine + jnp.sum(side_sums[...], axis=0)
    partner = side_sums[sides.index((0, 1))]
    result_ref[0:1, :] = mine * (1.0 / database)
    result_ref[1:2, :] = partner * (1.0 / database)
    result_ref[2:3, :] = all_sums * (1.0 / (database * everyone))

    sent = arrived.at[pl.ds(1, db - 1)]
    wait_bytes(sent, query_send)
    wait_bytes(landing, hit_send)
    wait_bytes(side_sums, side_send)


UNROLL = 4
ABSORB_UNROLL = 4


def place_outputs(result_ref, hits_ref, totals_ref):
    count = hits_ref.shape[1]
    for kind in range(3):
        first = result_ref[0:1, kind * count : (kind + 1) * count]
        second = result_ref[1:2, 16 + kind * count : 16 + (kind + 1) * count]
        hits_ref[kind : kind + 1, :] = first + second
    totals_ref[...] = result_ref[2:3, 64:67]


def solution(mesh):
    db, pb = mesh.shape["db"], mesh.shape["pb"]

    def per_device(queries, residual, codes, codebook, ranks):
        count, width = queries.shape
        rows = residual.shape[0]
        subspaces, centroids, subdim = codebook.shape
        sizes = (db, pb, rows, width, rows * db, count * pb * db, subdim)
        total = db * count
        in_vmem = pl.BlockSpec(memory_space=pltpu.VMEM)
        anywhere = pl.BlockSpec(memory_space=pl.ANY)
        dma = pltpu.SemaphoreType.DMA
        result = pl.pallas_call(
            lambda *refs: kernel_body(sizes, *refs),
            out_shape=pltpu.VMEM((8, LANES), jnp.float32),
            in_specs=[anywhere] * 5,
            out_specs=in_vmem,
            scratch_shapes=[
                pltpu.SMEM((count,), jnp.int32),
                pltpu.VMEM((count, width), jnp.bfloat16),
                pltpu.VMEM((count, width + LANES), jnp.bfloat16),
                pltpu.VMEM((db, count, width + LANES), jnp.bfloat16),
                pltpu.VMEM((subspaces, subdim, centroids), jnp.float32),
                pltpu.VMEM((subspaces, rows), jnp.int32),
                pltpu.VMEM((rows, width), jnp.bfloat16),
                pltpu.VMEM((width, rows), jnp.bfloat16),
                pltpu.VMEM((width, rows), jnp.bfloat16),
                pltpu.VMEM((8, rows), jnp.float32),
                pltpu.VMEM((8, rows), jnp.float32),
                pltpu.VMEM((total, width), jnp.bfloat16),
                pltpu.VMEM((total, LANES), jnp.float32),
                pltpu.VMEM((3, total, LANES), jnp.float32),
                pltpu.VMEM((total, LANES), jnp.int32),
                pltpu.VMEM((total, LANES), jnp.float32),
                pltpu.VMEM((NY * NZ, total), jnp.bfloat16),
                pltpu.VMEM((NY * NZ, 1, LANES), jnp.float32),
                pltpu.VMEM((NY * NZ, 1, LANES), jnp.float32),
                pltpu.VMEM((1, LANES), jnp.float32),
                pltpu.VMEM((pb * NX - 1, 1, LANES), jnp.float32),
                dma((5,)),
                dma,
                dma((NZ,)),
                dma((PLANE,)),
                dma((2,)),
                dma((2,)),
                dma,
                dma,
                dma,
                dma,
            ],
            compiler_params=pltpu.CompilerParams(
                collective_id=0, has_side_effects=True, vmem_limit_bytes=60 * 1024 * 1024
            ),
            name="recall",
        )(ranks, queries, residual, codes.T, jnp.transpose(codebook, (0, 2, 1)))
        hits, totals = pl.pallas_call(
            place_outputs,
            out_shape=(
                jax.ShapeDtypeStruct((3, count), jnp.float32),
                jax.ShapeDtypeStruct((1, 3), jnp.float32),
            ),
            in_specs=[in_vmem],
            name="place",
        )(pltpu.with_memory_space_constraint(result, pltpu.VMEM))
        return hits, totals.reshape(3)

    return jax.shard_map(
        per_device,
        mesh=mesh,
        in_specs=(P(("pb", "db"), None), P("db", None), P("db", None), P(), P(("pb", "db"))),
        out_specs=(P(None, ("pb", "db")), P()),
        check_vma=False,
    )
```
